32 devices in a mesh: section: 4 (over y, x), stem: 8 (over z, core).
Axes of the slice: x: 2, y: 2, z: 4, core: 2. Of those that a mesh axis runs over, the one named last changes fastest.
Arguments:
- bitstrings: int32 [4, 4, 32, 3], P('section'), may hold values 0 or 1
- boundary: float32 [2, 2048], replicated, may hold values from -6 to 6
- stem_tensor: float32 [4, 2, 2048, 8, 2048], P('section', None, 'stem'), may hold values from -0.09375 to 0.09375
- probe_vectors: float32 [4, 2, 2048], P('section'), may hold values from -0.09375 to 0.09375
- inbound_permutations: int32 [4, 2048], replicated, may hold values from 0 to 2047, each once within a row
Outputs:
- amplitudes: float32 [4, 2, 4, 32], P('section')
The draws below stay inside these ranges and needn't reach their ends.
Inputs may be any that keep to these rules, and one draw needn't show every extreme that they name: `inbound_permutations`: each row of relabeling names every number of 0 to 2047 once.
All inputs are finite; a program needn't handle non-finite values. No bound on the sum of `bitstrings` on one device may be relied on, other than what follows from the above.
Results may differ from the reference program's by a relative error of at most 0.0003.
Values sent between devices are 32-bit elements; how exact they have to be, the bound alone decides.
No kernel may reach another device: no remote copies, remote signals or barrier semaphores. Data moves between devices by JAX's collectives and lax.ppermute only.
A program may use at most 128 MiB of HBM per device.

```python
import jax
import jax.numpy as jnp
from jax import lax

K = 2048
QS = 3
P_SIZE = 8
B = 32
M = 4
N_SECTION = 4


def touch_ends(array, rng, least, top_value):
    longest = array.shape.index(max(array.shape))
    spots = []
    for shift in (0, 1):
        where = [jax.random.randint(jax.random.fold_in(rng, axis), (), 0, length) for axis, length in enumerate(array.shape)]
        where[longest] = (where[longest] + shift) % array.shape[longest]
        spots.append(tuple(where))
    return array.at[spots[0]].set(least).at[spots[1]].set(top_value)


def levels(stream_key, dims, cuts, low, top_value):
    gain = 1.0
    for dim, shards_of in cuts:
        draws = jax.random.uniform(jax.random.fold_in(jax.random.fold_in(stream_key, 6), dim), (shards_of,), jnp.float32, low / len(cuts), top_value / len(cuts))
        gain = gain * jnp.repeat(jnp.exp(draws), dims[dim] // shards_of).reshape((-1,) + (1,) * (len(dims) - 1 - dim))
    return gain


def scatter_about(rng, dims, spread, limit, pieces=(), kind=jnp.bfloat16):
    values = spread * jax.random.normal(rng, dims, jnp.float32)
    if pieces:
        values = values * levels(rng, dims, pieces, -0.22, 0.18)
    return jnp.clip(values, -limit, limit).astype(kind)


def setup_inputs(seed: int = 0) -> dict:
    key_of = jax.random.split(jax.random.key(seed), 6)
    bitstrings = touch_ends((jax.random.randint(key_of[0], (N_SECTION, M, B, QS), 0, 2) < 1).astype(jnp.int32), jax.random.fold_in(key_of[0], 1), 0, 1)
    boundary = scatter_about(key_of[1], (2, K), 1.0, 6.0, (), jnp.float32)
    stem_tensor = scatter_about(key_of[2], (N_SECTION, 2, K, P_SIZE, K), (2 * K) ** -0.5, 0.09375, ((0, 4), (2, 8)), jnp.float32)
    probe_vectors = scatter_about(key_of[3], (N_SECTION, 2, K), (2 * K) ** -0.5, 0.09375, ((0, 4),), jnp.float32)
    inbound_permutations = jax.vmap(lambda own: jax.random.permutation(own, K))(jax.random.split(key_of[4], N_SECTION)).reshape((N_SECTION, K)).astype(jnp.int32)
    return {"bitstrings": bitstrings, "boundary": boundary, "stem_tensor": stem_tensor, "probe_vectors": probe_vectors, "inbound_permutations": inbound_permutations}


def reference(bitstrings, boundary, stem_tensor, probe_vectors, inbound_permutations):
    powers = (2 ** jnp.arange(QS)).astype(jnp.int32)
    configuration_line = jnp.sum(bitstrings * powers, axis=-1).astype(jnp.int32)
    running_partial_vector = jnp.broadcast_to(boundary[:, None, None, :], (2, M, B, K)).astype(jnp.float32)
    collected = []
    for segment_ordinal in range(N_SECTION):
        reordered_factor = jnp.take(running_partial_vector, inbound_permutations[segment_ordinal], axis=3)
        flat_real = stem_tensor[segment_ordinal, 0].reshape(K * P_SIZE, K)
        flat_imag = stem_tensor[segment_ordinal, 1].reshape(K * P_SIZE, K)

        def forward_group_move(pair):
            vectors, pattern = pair
            onehot = (jnp.arange(P_SIZE).astype(jnp.int32)[None, :] == pattern[:, None]).astype(jnp.float32)
            expanded = (vectors[:, :, :, None] * onehot[None, :, None, :]).reshape(2 * B, K * P_SIZE)
            prod_real = jnp.dot(expanded, flat_real, precision=lax.Precision.HIGHEST)
            prod_imag = jnp.dot(expanded, flat_imag, precision=lax.Precision.HIGHEST)
            out_real = prod_real[:B] - prod_imag[B:]
            out_imag = prod_imag[:B] + prod_real[B:]
            return jnp.stack([out_real, out_imag])

        permuted_entries = lax.map(forward_group_move, (jnp.transpose(reordered_factor, (1, 0, 2, 3)), configuration_line[segment_ordinal]))
        running_partial_vector = jnp.transpose(permuted_entries, (1, 0, 2, 3))
        probe_re = probe_vectors[segment_ordinal, 0]
        probe_im = probe_vectors[segment_ordinal, 1]
        amp_real = jnp.dot(running_partial_vector[0], probe_re, precision=lax.Precision.HIGHEST) - jnp.dot(running_partial_vector[1], probe_im, precision=lax.Precision.HIGHEST)
        amp_imag = jnp.dot(running_partial_vector[0], probe_im, precision=lax.Precision.HIGHEST) + jnp.dot(running_partial_vector[1], probe_re, precision=lax.Precision.HIGHEST)
        collected.append(jnp.stack([amp_real, amp_imag]))
    return jnp.stack(collected)
```

```python
import functools

import jax
import jax.numpy as jnp
from jax import lax
from jax.experimental import pallas as pl
from jax.experimental.pallas import tpu as pltpu
from jax.sharding import Mesh
from jax.sharding import PartitionSpec as P


F32 = jnp.float32
BF16 = jnp.bfloat16
NT = (((1,), (1,)), ((), ()))
CHUNK = 32
TILE = 256


def split(x):
    high = x.astype(BF16)
    return high, (x - high.astype(F32)).astype(BF16)


def mm(a, b):
    return jnp.dot(a, b, preferred_element_type=F32)


def mm_nt(a, b):
    return lax.dot_general(a, b, NT, preferred_element_type=F32)


def iota(shape, dim):
    return lax.broadcasted_iota(jnp.int32, shape, dim)


def one_hot(cond):
    return jnp.where(cond, 1.0, 0.0).astype(BF16)


def repeat_matrix(rows, settings):
    shape = (rows, rows * settings)
    return one_hot(iota(shape, 1) // settings == iota(shape, 0))


def stage_body(first, settings, stem_count, role_ref, stem_ref, probe_ref, next_ref, *rest):
    if first:
        boundary_ref, rows_ref, block_out, amp_out = rest[:4]
        lhs_ref, acc_ref, back_lhs_ref, back_ref = rest[4:]
    else:
        recv_ref, keep_out, send_out, back_ref, amp_out = rest[:5]
        lhs_ref, acc_ref, back_lhs_ref = rest[5:]
    s8 = settings
    step = pl.program_id(0)
    last = pl.num_programs(0) - 1
    role = role_ref[0]
    width = probe_ref.shape[2]
    rows = lhs_ref.shape[2] // s8
    group = min(rows, 128)
    half = s8 * s8
    lanes = CHUNK * s8
    mask_shape = (2 * s8, group * s8)
    pick = (iota(mask_shape, 1) % s8) == (iota(mask_shape, 0) % s8)
    upper = iota(mask_shape, 0) < s8

    @pl.when((step == 0) & (role == 1))
    def _():
        acc_ref[...] = jnp.zeros(acc_ref.shape, F32)
        if first:
            b_hi, b_lo = split(boundary_ref[...])
            b_parts = jnp.concatenate([b_hi, b_lo, jnp.zeros((12, width), BF16)], 0)
            taken = []
            for start in range(0, rows, group):
                idx = rows_ref[:, start : start + group]
                total = jnp.zeros((16, group), F32)
                for j in range(0, width, TILE):
                    sel = one_hot(iota((TILE, group), 0) + j == idx)
                    total += mm(b_parts[:, j : j + TILE], sel)
                taken.append(total[0:2] + total[2:4])
        else:
            state = recv_ref[0]
            for d in range(1, stem_count):
                state += recv_ref[d]
        rep = repeat_matrix(group, s8)
        for g, start in enumerate(range(0, rows, group)):
            if first:
                part = jnp.concatenate(
                    [jnp.broadcast_to(taken[g][i : i + 1], (s8, group)) for i in (0, 1)], 0
                )
            else:
                part = state[:, start : start + group]
            hi, lo = split(part)
            wide = mm(jnp.concatenate([hi, lo], 0), rep)
            at = pl.ds(start * s8, group * s8)
            for level in range(2):
                for quarter in range(s8 // 2):
                    base = level * 2 * s8 + 2 * quarter
                    built = []
                    for plane in range(2):
                        r = base + plane * s8
                        value = jnp.where(upper, wide[r : r + 1], wide[r + 1 : r + 2])
                        built.append(jnp.where(pick, value, 0.0))
                    top = level * 2 * half + quarter * 4 * s8
                    lo_rows = pl.ds(top, 2 * s8)
                    hi_rows = pl.ds(top + 2 * s8, 2 * s8)
                    lhs_ref[0, lo_rows, at] = built[0].astype(BF16)
                    lhs_ref[0, hi_rows, at] = built[1].astype(BF16)
                    lhs_ref[1, lo_rows, at] = (-built[1]).astype(BF16)
                    lhs_ref[1, hi_rows, at] = built[0].astype(BF16)

    @pl.when((step == 0) & (role == 2))
    def _():
        zero = jnp.zeros((s8 - 1, width), F32)
        if first:
            front = [jnp.zeros((s8, width), F32)] * 2
        else:
            pieces = [split(recv_ref[d]) for d in range(stem_count)]
            parts = jnp.concatenate(
                [jnp.concatenate([p[i] for p in pieces], 1) for i in (0, 1)], 0
            )
            moved = []
            for j in range(0, width, TILE):
                total = jnp.zeros((4 * s8, TILE), F32)
                for k in range(0, width, TILE):
                    sel = one_hot(iota((TILE, TILE), 0) + j == next_ref[:, k : k + TILE])
                    total += mm_nt(parts[:, k : k + TILE], sel)
                moved.append(total[: 2 * s8] + total[2 * s8 :])
            moved = jnp.concatenate(moved, 1)
            front = [moved[:s8], moved[s8:]]
        real = jnp.concatenate([front[0], probe_ref[0, 0:1], zero], 0)
        imag = jnp.concatenate([front[1], probe_ref[0, 1:2], zero], 0)
        for plane, pair in enumerate([(real, imag), (-imag, real)]):
            hi, lo = split(jnp.concatenate(pair, 0))
            back_lhs_ref[plane, 0 : 4 * s8] = hi
            back_lhs_ref[plane, 4 * s8 :] = lo

    @pl.when(role == 1)
    def _():
        at = pl.ds(pl.multiple_of(step * lanes, lanes), lanes)
        for j in range(0, width, 2 * TILE):
            total = acc_ref[:, j : j + 2 * TILE]
            extra = jnp.zeros((2 * half, 2 * TILE), F32)
            for plane in range(2):
                t = stem_ref[0, plane, :, :, j : j + 2 * TILE].reshape(lanes, 2 * TILE)
                hi, lo = split(t)
                e = lhs_ref[plane, :, at]
                total += mm(e, hi)
                extra += mm(e[: 2 * half], lo)
            acc_ref[0 : 2 * half, j : j + 2 * TILE] = total[: 2 * half] + extra
            acc_ref[2 * half :, j : j + 2 * TILE] = total[2 * half :]

    @pl.when(role == 2)
    def _():
        total = jnp.zeros((8 * s8, lanes), F32)
        extra = jnp.zeros((4 * s8, lanes), F32)
        for plane in range(2):
            t = stem_ref[0, plane].reshape(lanes, width)
            hi, lo = split(t)
            total += mm_nt(back_lhs_ref[plane], hi)
            extra += mm_nt(back_lhs_ref[plane, 0 : 4 * s8], lo)
        at = pl.ds(pl.multiple_of(step * lanes, lanes), lanes)
        back_ref[:, at] = total[: 4 * s8] + total[4 * s8 :] + extra

    @pl.when((step == last) & (role == 1))
    def _():
        used = 4 * s8 if first else 2 * half
        full = acc_ref[0 : 2 * half] + acc_ref[2 * half :]
        f_hi, f_lo = split(full)
        p_hi, p_lo = split(probe_ref[0])
        lhs = jnp.concatenate([p_hi, p_lo, jnp.zeros((12, width), BF16)], 0)
        by_hi = mm_nt(lhs, f_hi)
        by_lo = mm_nt(lhs, f_lo)
        amps = by_hi[0:2] + by_hi[2:4] + by_lo[0:2]
        amp_out[...] = jnp.concatenate([amps, jnp.zeros((6, 2 * half), F32)], 0)
        parts = jnp.concatenate([f_hi[:used], f_lo[:used]], 0)
        for i in range(0, width, TILE):
            total = jnp.zeros((2 * used, TILE), F32)
            for j in range(0, width, TILE):
                sel = one_hot(iota((TILE, TILE), 0) + j == next_ref[:, i : i + TILE])
                total += mm(parts[:, j : j + TILE], sel)
            moved = total[:used] + total[used:]
            if first:
                wanted = jnp.concatenate([moved[0:s8], moved[2 * s8 : 3 * s8]], 0)
                if rows <= TILE:
                    for o in range(0, TILE, rows):
                        block_out[(i + o) // rows] = wanted[:, o : o + rows]
                else:
                    block_out[i // rows, :, i % rows : i % rows + TILE] = wanted
            elif i < width // 2:
                keep_out[:, i : i + TILE] = moved
            else:
                send_out[:, i - width // 2 : i - width // 2 + TILE] = moved

    if first:

        @pl.when((step == last) & (role == 2))
        def _():
            rep = repeat_matrix(group, s8)
            for start in range(0, rows, group):
                at = slice(start * s8, (start + group) * s8)
                real = jnp.broadcast_to(back_ref[s8 : s8 + 1, at], mask_shape)
                imag = jnp.broadcast_to(back_ref[3 * s8 : 3 * s8 + 1, at], mask_shape)
                spread = jnp.where(pick, jnp.where(upper, real, imag), 0.0)
                hi, lo = split(spread)
                out = mm_nt(hi, rep) + mm_nt(lo, rep)
                for d in range(stem_count):
                    block_out[d, :, start : start + group] = out


def final_body(settings, section_count, scalars_ref, u_ref, x_ref, set_ref, amp0_ref, amp1_ref, out_ref):
    s8 = settings
    section = scalars_ref[0]
    half = s8 * s8
    rows = u_ref.shape[2]
    count = set_ref.shape[1]
    u = u_ref[0]
    for z in range(1, u_ref.shape[0]):
        u += u_ref[z]
    group = min(rows, 128)
    rep = repeat_matrix(group, s8)
    shape = (s8, group * s8)
    pick = (iota(shape, 1) % s8) == iota(shape, 0)
    table = jnp.zeros((4 * s8, 4 * half), F32)
    for start in range(0, rows, group):
        hi, lo = split(u[:, start : start + group])
        wide = mm(jnp.concatenate([hi, lo], 0), rep)
        spread = []
        for level in range(2):
            tiles = [
                jnp.where(pick, wide[r : r + 1], 0.0)
                for r in range(level * 4 * s8, (level + 1) * 4 * s8)
            ]
            spread.append(jnp.concatenate(tiles, 0).astype(BF16))
        x_hi, x_lo = split(x_ref[:, start * s8 : (start + group) * s8])
        both = mm_nt(jnp.concatenate([x_hi, x_lo], 0), spread[0])
        table += both[: 4 * s8] + both[4 * s8 :] + mm_nt(x_hi, spread[1])
    per = 2 * s8 * s8
    re_u, im_u = table[:, :per], table[:, per:]
    c_re = re_u[: 2 * s8] - im_u[2 * s8 :]
    c_im = re_u[2 * s8 :] + im_u[: 2 * s8]
    sets = set_ref[...]
    s = [sets[i : i + 1] for i in range(section_count)]
    quarter = s[0] // 2
    code = ((s[0] % 2) * s8 + s[1]) * s8 + s[2]
    sel = one_hot((iota((per, count), 0) == code) & (quarter == section))
    parts = split(jnp.concatenate([c_re, c_im], 0))
    chosen = mm(parts[0], sel) + mm(parts[1], sel)
    match = iota((s8, count), 0) == s[3]
    for plane in range(2):
        top = plane * 2 * s8
        amp3 = jnp.sum(jnp.where(match, chosen[top : top + s8], 0.0), 0, keepdims=True)
        out_ref[3, plane : plane + 1] = amp3
        out_ref[2, plane : plane + 1] = chosen[top + s8 : top + s8 + 1]
    for target, ref in ((0, amp0_ref), (1, amp1_ref)):
        first_set, second_set = (s[0] * 0, s[0]) if target == 0 else (s[0], s[1])
        place = (first_set // 2) * (4 * s8) + (first_set % 2) * s8 + second_set
        at = iota((2 * half, count), 0)
        pair = split(ref[...])
        picked = []
        for shift in (0, 2 * s8):
            oh = one_hot(at == place + shift)
            picked.append(mm(pair[0], oh) + mm(pair[1], oh))
        real = picked[0][0:1] - picked[1][1:2]
        imag = picked[0][1:2] + picked[1][0:1]
        mine = section == target
        out_ref[target, 0:1] = jnp.where(mine, real, 0.0)
        out_ref[target, 1:2] = jnp.where(mine, imag, 0.0)


def local(bitstrings, boundary, stem_tensor, probe_vectors, inbound_permutations):
    rows, s8, width = stem_tensor.shape[2:]
    micro, batch, qubits = bitstrings.shape[1:]
    count = micro * batch
    section_count = lax.axis_size("a") * lax.axis_size("b")
    z_count = lax.axis_size("z")
    stem_count = z_count * 2
    assert section_count == 4 and s8 == 2 * section_count
    every = ("a", "b", "z", "c")
    section = lax.axis_index("a") * lax.axis_size("b") + lax.axis_index("b")
    core = lax.axis_index("c")
    stem_rank = lax.axis_index("z") * 2 + core
    half = s8 * s8

    powers = jnp.left_shift(jnp.int32(1), jnp.arange(qubits, dtype=jnp.int32))
    own_setting = jnp.sum(bitstrings[0] * powers, axis=-1).reshape(1, count)
    own_perm = lax.dynamic_index_in_dim(inbound_permutations, section, 0, True)
    following = jnp.minimum(section + 1, section_count - 1)
    next_perm = lax.dynamic_index_in_dim(inbound_permutations, following, 0, True)
    row_ids = lax.dynamic_slice_in_dim(own_perm, stem_rank * rows, rows, 1)
    by_core = next_perm.reshape(z_count, 2, rows).transpose(1, 0, 2)
    kept = jnp.where(core == 0, by_core[0], by_core[1]).reshape(1, width // 2)
    sent = jnp.where(core == 0, by_core[1], by_core[0]).reshape(1, width // 2)
    swapped_perm = jnp.concatenate([kept, sent], 1)

    chunks = rows // CHUNK

    def stage(first, role, operands, operand_specs, out_shapes, out_specs, scratch):
        def stem_map(i, role_ref):
            return (0, 0, jnp.where(role_ref[0] > 0, i, 0), 0, 0)

        whole = lambda shape: pl.BlockSpec(shape, lambda i, r: (0,) * len(shape))
        return pl.pallas_call(
            functools.partial(stage_body, first, s8, stem_count),
            out_shape=out_shapes,
            grid_spec=pltpu.PrefetchScalarGridSpec(
                num_scalar_prefetch=1,
                grid=(chunks,),
                in_specs=[
                    pl.BlockSpec((1, 2, CHUNK, s8, width), stem_map),
                    whole((1, 2, width)),
                    whole((1, width)),
                ]
                + [whole(s) for s in operand_specs],
                out_specs=[whole(s) for s in out_specs],
                scratch_shapes=scratch,
            ),
            compiler_params=pltpu.CompilerParams(
                dimension_semantics=("arbitrary",), vmem_limit_bytes=60 * 2**20
            ),
            name="stage_a" if first else "stage_b",
        )(role, stem_tensor, probe_vectors, *operands)

    scratch = [
        pltpu.VMEM((2, 4 * half, rows * s8), BF16),
        pltpu.VMEM((4 * half, width), F32),
        pltpu.VMEM((2, 8 * s8, width), BF16),
    ]
    sds = jax.ShapeDtypeStruct
    role_a = jnp.where(section == 0, 1, jnp.where(section == 3, 2, 0)).reshape(1)
    blocks, amp0 = stage(
        True,
        role_a,
        (next_perm, boundary, row_ids),
        [(2, width), (1, rows)],
        [sds((stem_count, 2 * s8, rows), F32), sds((8, 2 * half), F32)],
        [(stem_count, 2 * s8, rows), (8, 2 * half)],
        scratch + [pltpu.VMEM((4 * s8, rows * s8), F32)],
    )
    doubled = jnp.concatenate([blocks, blocks], 0)
    swapped = lax.all_to_all(doubled, ("b", "z", "c"), 0, 0, tiled=True)
    recv = jnp.where(lax.axis_index("b") == 0, swapped[stem_count:], swapped[:stem_count])

    perm_b = jnp.where(section == 2, next_perm, swapped_perm)
    role_b = jnp.where(section == 1, 1, jnp.where(section == 2, 2, 0)).reshape(1)
    keep, send, back, amp1 = stage(
        False,
        role_b,
        (perm_b, recv),
        [(stem_count, 2 * s8, rows)],
        [
            sds((2 * half, width // 2), F32),
            sds((2 * half, width // 2), F32),
            sds((4 * s8, rows * s8), F32),
            sds((8, 2 * half), F32),
        ],
        [
            (2 * half, width // 2),
            (2 * half, width // 2),
            (4 * s8, rows * s8),
            (8, 2 * half),
        ],
        scratch,
    )
    u_half = keep + lax.ppermute(send, "c", [(0, 1), (1, 0)])

    span = width // 2
    wide = rows * s8
    nine = jnp.concatenate([back[: s8 + 8], back[2 * s8 : 3 * s8 + 8]], 0)
    vectors = jnp.concatenate([back[:s8], back[2 * s8 : 3 * s8]], 0)
    probes = jnp.concatenate([back[s8 : s8 + 1], back[3 * s8 : 3 * s8 + 1]], 0)

    def fold(x):
        if wide <= span:
            return jnp.pad(x, ((0, 0), (0, span - wide)))
        return jnp.concatenate([x[:, i : i + span] for i in range(0, wide, span)], 0)

    def unfold(x, count_rows):
        if wide <= span:
            return x[:count_rows, :wide]
        return jnp.concatenate(
            [x[i * count_rows : (i + 1) * count_rows] for i in range(wide // span)], 1
        )

    folds = max(wide // span, 1)
    x_rows = 2 * s8 * folds
    u_rows = 4 * s8
    body_rows = max(x_rows, u_rows)
    pad_rows = lambda x, n: jnp.pad(x, ((0, n - x.shape[0]), (0, 0)))
    set_row = jnp.pad(own_setting.astype(F32), ((0, 0), (0, span - count)))
    tail = pad_rows(jnp.concatenate([set_row, fold(probes)], 0), 8)
    x_pay = pad_rows(fold(vectors), body_rows)

    def payload(quarter):
        u_pay = pad_rows(u_half[quarter * u_rows : (quarter + 1) * u_rows], body_rows)
        return jnp.concatenate([jnp.where(section == 2, x_pay, u_pay), tail], 0)

    sections = range(section_count)
    got = [payload(1)]
    for d in range(1, section_count):
        route = [(i * stem_count + r, (i ^ d) * stem_count + r) for i in sections for r in range(stem_count)]
        got.append(lax.ppermute(payload(1 ^ d), every, route))

    def choose(items, index):
        out = items[0]
        for i in range(1, len(items)):
            out = jnp.where(index == i, items[i], out)
        return out

    u_quarter = choose([g[:u_rows] for g in got], section ^ 1)
    x_all = choose(got, section ^ 2)
    all_sets = [choose([g[body_rows : body_rows + 1, :count] for g in got], section ^ i) for i in sections]
    sets = jnp.concatenate(all_sets, 0).astype(jnp.int32)
    x_vec = unfold(x_all[:x_rows], 2 * s8)
    x_prb = unfold(x_all[body_rows + 1 :], 2)
    blank = jnp.zeros((s8 - 1, wide), F32)
    x_full = jnp.concatenate([x_vec[:s8], x_prb[0:1], blank, x_vec[s8:], x_prb[1:2], blank], 0)

    u_split = u_quarter.reshape(u_rows, z_count, rows).transpose(1, 0, 2)
    u_recv = lax.all_to_all(u_split, "z", 0, 0, tiled=True)

    contrib = pl.pallas_call(
        functools.partial(final_body, s8, section_count),
        out_shape=sds((section_count, 2, count), F32),
        in_specs=[pl.BlockSpec(memory_space=pltpu.SMEM)] + [pl.BlockSpec(memory_space=pltpu.VMEM)] * 5,
        out_specs=pl.BlockSpec(memory_space=pltpu.VMEM),
        name="final",
    )(section.reshape(1), u_recv, x_full, sets, amp0, amp1)

    outgoing = jnp.broadcast_to(contrib[:, None], (section_count, stem_count, 2, count))
    outgoing = outgoing.reshape(section_count * stem_count, 2, count)
    arrived = lax.all_to_all(outgoing, every, 0, 0, tiled=True)
    return jnp.sum(arrived, 0).reshape(1, 2, micro, batch)


def solution(mesh):
    sections, stems = (mesh.shape[name] for name in ("section", "stem"))
    devices = mesh.devices.reshape(sections // 2, 2, stems // 2, 2)
    fine = Mesh(devices, ("a", "b", "z", "c"))
    return jax.shard_map(
        local,
        mesh=fine,
        in_specs=(
            P(("a", "b")),
            P(),
            P(("a", "b"), None, ("z", "c")),
            P(("a", "b")),
            P(),
        ),
        out_specs=P(("a", "b")),
        check_vma=False,
    )
```

```python
import functools

import jax
import jax.numpy as jnp
from jax import lax
from jax.experimental import pallas as pl
from jax.experimental.pallas import tpu as pltpu
from jax.sharding import Mesh
from jax.sharding import PartitionSpec as P


F32 = jnp.float32
BF16 = jnp.bfloat16
NT = (((1,), (1,)), ((), ()))
CHUNK = 32
TILE = 256
ROW_TILE = 8


def split(x):
    high = x.astype(BF16)
    return high, (x - high.astype(F32)).astype(BF16)


def mm(a, b):
    return jnp.dot(a, b, preferred_element_type=F32)


def mm_nt(a, b):
    return lax.dot_general(a, b, NT, preferred_element_type=F32)


def iota(shape, dim):
    return lax.broadcasted_iota(jnp.int32, shape, dim)


def one_hot(cond):
    return jnp.where(cond, 1.0, 0.0).astype(BF16)


def repeat_matrix(rows, settings):
    shape = (rows, rows * settings)
    return one_hot(iota(shape, 1) // settings == iota(shape, 0))


def position():
    section = lax.axis_index("a") * lax.axis_size("b") + lax.axis_index("b")
    core = lax.axis_index("c")
    rank = lax.axis_index("z") * lax.axis_size("c") + core
    return section, rank, core


def chunk_copy(stem_hbm, bufs, sem, b, i):
    held = bufs[b].shape[1]
    source = stem_hbm.at[0, :, pl.ds(b * held + i * CHUNK, CHUNK)]
    slot = sem.at[b * (held // CHUNK) + i]
    return pltpu.make_async_copy(source, bufs[b].at[:, pl.ds(i * CHUNK, CHUNK)], slot)


def permuted_tiles(parts, hot_ref, store):
    count = parts.shape[0] // 2
    for i in range(0, hot_ref.shape[1], TILE):
        total = mm(parts, hot_ref[:, i : i + TILE])
        store(i, total[:count] + total[count:])


def probe_amplitudes(probe, vectors):
    p_hi, p_lo = split(probe)
    lhs = jnp.concatenate([p_hi, p_lo, jnp.zeros((12, probe.shape[1]), BF16)], 0)
    v_hi, v_lo = split(vectors)
    by_hi, by_lo = mm_nt(lhs, v_hi), mm_nt(lhs, v_lo)
    return by_hi[0:2] + by_hi[2:4] + by_lo[0:2]


def first_body(buffers, boundary_hbm, perm_hbm, stem_hbm, probe_hbm, bits_ref, block_out, amp_out, set_out, hot_out, *rest):
    bufs = rest[:buffers]
    boundary_smem, perm_smem, probe_ref, perm_ref, small, sem, fwd_ref, part_ref, back_ref = rest[buffers:]
    section, rank, core = position()
    held, s8, width = bufs[0].shape[1:]
    rows = held * buffers
    per = held // CHUNK
    lanes = CHUNK * s8
    stem_count = block_out.shape[0] // 2
    target = (1 - lax.axis_index("b")) * stem_count
    pairs = [
        (perm_hbm, perm_ref),
        (boundary_hbm, boundary_smem),
        (perm_hbm, perm_smem),
        (probe_hbm, probe_ref),
    ]
    little = [pltpu.make_async_copy(a, b, small.at[i]) for i, (a, b) in enumerate(pairs)]
    for copy in little:
        copy.start()
    for b in range(buffers):
        for i in range(per):
            chunk_copy(stem_hbm, bufs, sem, b, i).start()
    settings = bits_ref[0]
    for q in range(1, bits_ref.shape[0]):
        settings += jnp.left_shift(bits_ref[q], q)
    line = jnp.concatenate([settings[i : i + 1] for i in range(settings.shape[0])], 1)
    set_out[...] = jnp.broadcast_to(line.astype(F32), set_out.shape)
    for copy in little:
        copy.wait()

    @pl.when(section <= 1)
    def _():
        wanted = perm_ref[pl.ds(section + 1, 1)]
        parts = [wanted[:, d * rows : (d + 1) * rows] for d in range(stem_count)]
        kept_first = [jnp.concatenate(parts[c::2] + parts[1 - c :: 2], 1) for c in (0, 1)]
        swapped = jnp.where(core == 0, kept_first[0], kept_first[1])
        perm_ref[0:1] = jnp.where(section == 1, swapped, wanted)

        def place(i, carry):
            at = pl.ds(pl.multiple_of(i * TILE, TILE), TILE)
            row = perm_ref[0:1, at]
            for j in range(0, width, TILE):
                hot_out[j : j + TILE, at] = one_hot(iota((TILE, TILE), 0) + j == row)
            return carry

        lax.fori_loop(0, width // TILE, place, 0)

    @pl.when(section == 2)
    def _():
        def place(i, carry):
            at = pl.ds(pl.multiple_of(i * 128, 128), 128)
            wanted = jnp.broadcast_to(perm_ref[3:4, at], (128, 128)).astype(F32).T
            for j in range(0, width, 128):
                place_at = (iota((128, 128), 1) + j).astype(F32)
                hot_out[at, j : j + 128] = one_hot(place_at == wanted)
            return carry

        lax.fori_loop(0, width // 128, place, 0)

    @pl.when((section == 1) | (section == 2))
    def _():
        for b in range(buffers):
            for i in range(per):
                chunk_copy(stem_hbm, bufs, sem, b, i).wait()

    @pl.when(section == 0)
    def _():
        fwd_ref[...] = jnp.zeros(fwd_ref.shape, F32)
        piece = min(width, 1024)

        def chunk(b, c, carry):
            chunk_copy(stem_hbm, bufs, sem, b, c).wait()
            for j in range(0, width, piece):
                at = slice(j, j + piece)

                def one(i, sums):
                    k = c * CHUNK + i
                    source = perm_smem[0, rank * rows + b * held + k]
                    b_re, b_im = boundary_smem[0, source], boundary_smem[1, source]
                    t_re, t_im = bufs[b][0, k, :, at], bufs[b][1, k, :, at]
                    return sums[0] + (b_re * t_re - b_im * t_im), sums[1] + (b_re * t_im + b_im * t_re)

                start = fwd_ref[0:s8, at], fwd_ref[s8:, at]
                done = lax.fori_loop(0, CHUNK, one, start, unroll=4)
                fwd_ref[0:s8, at], fwd_ref[s8:, at] = done
            return carry

        for b in range(buffers):
            lax.fori_loop(0, per, functools.partial(chunk, b), 0)
        full = fwd_ref[...]
        gap = jnp.zeros((s8, width), F32)
        spaced = jnp.concatenate([full[:s8], gap, full[s8:], gap], 0)
        amps = probe_amplitudes(probe_ref[0], spaced)
        amp_out[...] = jnp.zeros(amp_out.shape, F32)
        amp_out[0:2, 0 : 4 * s8] = amps

        def store(i, moved):
            if rows <= TILE:
                for o in range(0, TILE, rows):
                    block_out[target + (i + o) // rows] = moved[:, o : o + rows]
            else:
                block_out[target + i // rows, :, i % rows : i % rows + TILE] = moved

        permuted_tiles(jnp.concatenate(split(full), 0), hot_out, store)

    @pl.when(section == 3)
    def _():
        ones = jnp.ones((s8, 128), BF16)
        quarters = 4
        span = width // 128 // quarters

        def chunk(b, c, carry):
            chunk_copy(stem_hbm, bufs, sem, b, c).wait()
            for q in range(quarters):
                tiles = [slice(128 * t, 128 * t + 128) for t in range(q * span, (q + 1) * span)]
                p_re = [jnp.broadcast_to(probe_ref[0, 0:1, t], (s8, 128)) for t in tiles]
                p_im = [jnp.broadcast_to(probe_ref[0, 1:2, t], (s8, 128)) for t in tiles]

                def one(i, carry):
                    k = c * CHUNK + i
                    re, im = None, None
                    for n, t in enumerate(tiles):
                        t_re, t_im = bufs[b][0, k, :, t], bufs[b][1, k, :, t]
                        r = t_re * p_re[n] - t_im * p_im[n]
                        m = t_re * p_im[n] + t_im * p_re[n]
                        re, im = (r, m) if re is None else (re + r, im + m)
                    at = pl.ds(pl.multiple_of(i * s8, s8), s8)
                    if q == 0:
                        part_ref[at, 0:128], part_ref[at, 128:] = re, im
                    else:
                        part_ref[at, 0:128] += re
                        part_ref[at, 128:] += im
                    return carry

                lax.fori_loop(0, CHUNK, one, 0, unroll=8)
            hi, lo = split(part_ref[...])
            at = pl.ds(pl.multiple_of((b * per + c) * lanes, lanes), lanes)
            for plane in range(2):
                side = slice(128 * plane, 128 * plane + 128)
                back_ref[s8 * plane : s8 * plane + s8, at] = mm_nt(ones, hi[:, side]) + mm_nt(ones, lo[:, side])
            return carry

        for b in range(buffers):
            lax.fori_loop(0, per, functools.partial(chunk, b), 0)
        group = min(rows, 128)
        rep = repeat_matrix(group, s8)
        shape = (2 * s8, group * s8)
        pick = (iota(shape, 1) % s8) == (iota(shape, 0) % s8)
        for start in range(0, rows, group):
            spread = jnp.where(pick, back_ref[:, start * s8 : (start + group) * s8], 0.0)
            hi, lo = split(spread)
            out = mm_nt(hi, rep) + mm_nt(lo, rep)
            for d in range(stem_count):
                block_out[target + d, :, start : start + group] = out


def second_body(buffers, *refs):
    bufs = refs[:buffers]
    recv_ref, hot_ref, probe_ref, set_ref, keep_out, send_out, amp_out = refs[buffers : buffers + 7]
    lhs_ref, acc_ref, back_lhs_ref, back_ref = refs[buffers + 7 :]
    section, _, _ = position()
    held, s8, width = bufs[0].shape[1:]
    rows = held * buffers
    count = rows // CHUNK
    per = held // CHUNK
    lanes = CHUNK * s8
    half = s8 * s8
    stem_count = recv_ref.shape[0] // 2
    body = 4 * s8 * (stem_count // 2)
    source = (1 - lax.axis_index("b")) * stem_count
    group = min(rows, 128)
    batch = set_ref.shape[1]

    for q in range(keep_out.shape[0]):
        for i, at in enumerate(range(0, batch, rows)):
            n = min(rows, batch - at)
            keep_out[q, body + 2 * s8 + i : body + 2 * s8 + i + 1, 0:n] = set_ref[0:1, at : at + n]

    @pl.when(section == 1)
    def _():
        acc_ref[...] = jnp.zeros(acc_ref.shape, F32)
        state = recv_ref[source]
        for d in range(1, stem_count):
            state += recv_ref[source + d]
        rep = repeat_matrix(group, s8)
        mask_shape = (2 * s8, group * s8)
        pick = (iota(mask_shape, 1) % s8) == (iota(mask_shape, 0) % s8)
        upper = iota(mask_shape, 0) < s8
        for start in range(0, rows, group):
            hi, lo = split(state[:, start : start + group])
            wide = mm(jnp.concatenate([hi, lo], 0), rep)
            at = pl.ds(start * s8, group * s8)
            for level in range(2):
                for quarter in range(s8 // 2):
                    base = level * 2 * s8 + 2 * quarter
                    built = []
                    for plane in range(2):
                        r = base + plane * s8
                        value = jnp.where(upper, wide[r : r + 1], wide[r + 1 : r + 2])
                        built.append(jnp.where(pick, value, 0.0))
                    top = level * 2 * half + quarter * 4 * s8
                    lo_rows = pl.ds(top, 2 * s8)
                    hi_rows = pl.ds(top + 2 * s8, 2 * s8)
                    lhs_ref[0, lo_rows, at] = built[0].astype(BF16)
                    lhs_ref[0, hi_rows, at] = built[1].astype(BF16)
                    lhs_ref[1, lo_rows, at] = (-built[1]).astype(BF16)
                    lhs_ref[1, hi_rows, at] = built[0].astype(BF16)

        for c in range(count):
            at = slice(c * lanes, (c + 1) * lanes)
            ks = slice(c % per * CHUNK, (c % per + 1) * CHUNK)
            for j in range(0, width, 2 * TILE):
                cols = slice(j, j + 2 * TILE)
                total = acc_ref[:, cols]
                extra = jnp.zeros((2 * half, 2 * TILE), F32)
                for plane in range(2):
                    hi, lo = split(bufs[c // per][plane, ks, :, cols].reshape(lanes, 2 * TILE))
                    e = lhs_ref[plane, :, at]
                    total += mm(e, hi)
                    extra += mm(e[: 2 * half], lo)
                acc_ref[0 : 2 * half, cols] = total[: 2 * half] + extra
                acc_ref[2 * half :, cols] = total[2 * half :]
        full = acc_ref[0 : 2 * half] + acc_ref[2 * half :]
        amp_out[0:2] = probe_amplitudes(probe_ref[0], full)

        def store(i, moved):
            n = min(rows, TILE)
            for o in range(0, TILE, n):
                slot, lane = divmod(i + o, rows)
                z, ref = slot % (stem_count // 2), (keep_out, send_out)[slot // (stem_count // 2)]
                for q in range(s8 // 2):
                    piece = moved[q * 4 * s8 : (q + 1) * 4 * s8, o : o + n]
                    ref[q, z * 4 * s8 : (z + 1) * 4 * s8, lane : lane + n] = piece

        permuted_tiles(jnp.concatenate(split(full), 0), hot_ref, store)

    @pl.when(section == 2)
    def _():
        zero = jnp.zeros((s8 - 1, width), F32)
        pieces = [split(recv_ref[source + d]) for d in range(stem_count)]
        parts = jnp.concatenate([jnp.concatenate([p[i] for p in pieces], 1) for i in (0, 1)], 0)
        moved = []
        permuted_tiles(parts, hot_ref, lambda i, x: moved.append(x))
        moved = jnp.concatenate(moved, 1)
        real = jnp.concatenate([moved[:s8], probe_ref[0, 0:1], zero], 0)
        imag = jnp.concatenate([moved[s8:], probe_ref[0, 1:2], zero], 0)
        for plane, pair in enumerate([(real, imag), (-imag, real)]):
            hi, lo = split(jnp.concatenate(pair, 0))
            back_lhs_ref[plane, 0 : 4 * s8] = hi
            back_lhs_ref[plane, 4 * s8 :] = lo

        for c in range(count):
            ks = slice(c % per * CHUNK, (c % per + 1) * CHUNK)
            total = jnp.zeros((8 * s8, lanes), F32)
            extra = jnp.zeros((4 * s8, lanes), F32)
            for plane in range(2):
                hi, lo = split(bufs[c // per][plane, ks].reshape(lanes, width))
                total += mm_nt(back_lhs_ref[plane], hi)
                extra += mm_nt(back_lhs_ref[plane, 0 : 4 * s8], lo)
            at = slice(c * lanes, (c + 1) * lanes)
            back_ref[:, at] = total[: 4 * s8] + total[4 * s8 :] + extra
        for i in range(s8):
            at = slice(i * rows, (i + 1) * rows)
            for q in range(keep_out.shape[0]):
                for plane in range(2):
                    row = 2 * s8 * (i) + plane * s8
                    keep_out[q, row : row + s8, :] = back_ref[2 * s8 * plane : 2 * s8 * plane + s8, at]
                    row = body + 2 * i + plane
                    src = 2 * s8 * plane + s8
                    keep_out[q, row : row + 1, :] = back_ref[src : src + 1, at]


def pack_body(keep_ref, recv_ref, out_ref):
    section, _, _ = position()

    @pl.when(section == 1)
    def _():
        out_ref[...] = keep_ref[...] + recv_ref[...]
        tail = keep_ref.shape[1] - ROW_TILE
        out_ref[:, tail:] = keep_ref[:, tail:]

    @pl.when(section != 1)
    def _():
        out_ref[...] = keep_ref[...]


def final_body(settings, u_ref, got_ref, amp0_ref, amp1_ref, out_ref, x_ref):
    s8 = settings
    section, _, _ = position()
    half = s8 * s8
    section_count = got_ref.shape[0]
    rows = u_ref.shape[2]
    count = out_ref.shape[2]
    body = u_ref.shape[0] * 4 * s8
    u = u_ref[0]
    for z in range(1, u_ref.shape[0]):
        u += u_ref[z]
    x_ref[...] = jnp.zeros(x_ref.shape, F32)
    for i in range(s8):
        at = slice(i * rows, (i + 1) * rows)
        for plane in range(2):
            row = 2 * s8 * i + plane * s8
            x_ref[2 * s8 * plane : 2 * s8 * plane + s8, at] = got_ref[2, row : row + s8]
            row = body + 2 * i + plane
            to = 2 * s8 * plane + s8
            x_ref[to : to + 1, at] = got_ref[2, row : row + 1]
    group = min(rows, 128)
    rep = repeat_matrix(group, s8)
    shape = (s8, group * s8)
    pick = (iota(shape, 1) % s8) == iota(shape, 0)
    table = jnp.zeros((4 * s8, 4 * half), F32)
    for start in range(0, rows, group):
        hi, lo = split(u[:, start : start + group])
        wide = mm(jnp.concatenate([hi, lo], 0), rep)
        spread = []
        for level in range(2):
            tiles = [
                jnp.where(pick, wide[r : r + 1], 0.0)
                for r in range(level * 4 * s8, (level + 1) * 4 * s8)
            ]
            spread.append(jnp.concatenate(tiles, 0).astype(BF16))
        x_hi, x_lo = split(x_ref[:, start * s8 : (start + group) * s8])
        both = mm_nt(jnp.concatenate([x_hi, x_lo], 0), spread[0])
        table += both[: 4 * s8] + both[4 * s8 :] + mm_nt(x_hi, spread[1])
    per = 2 * s8 * s8
    re_u, im_u = table[:, :per], table[:, per:]
    c_re = re_u[: 2 * s8] - im_u[2 * s8 :]
    c_im = re_u[2 * s8 :] + im_u[: 2 * s8]
    top = body + 2 * s8
    s = []
    for i in range(section_count):
        pieces = [
            got_ref[i, top + n : top + n + 1, 0 : min(rows, count - at)]
            for n, at in enumerate(range(0, count, rows))
        ]
        s.append(jnp.concatenate(pieces, 1).astype(jnp.int32))
    code = ((s[0] % 2) * s8 + s[1]) * s8 + s[2]
    sel = one_hot((iota((per, count), 0) == code) & (s[0] // 2 == section))
    parts = split(jnp.concatenate([c_re, c_im], 0))
    chosen = mm(parts[0], sel) + mm(parts[1], sel)
    match = iota((s8, count), 0) == s[3]
    result = [[None, None] for _ in range(section_count)]
    for plane in range(2):
        top = plane * 2 * s8
        result[3][plane] = jnp.sum(jnp.where(match, chosen[top : top + s8], 0.0), 0, keepdims=True)
        result[2][plane] = chosen[top + s8 : top + s8 + 1]
    for target, ref in ((0, amp0_ref), (1, amp1_ref)):
        first_set, second_set = (s[0] * 0, s[0]) if target == 0 else (s[0], s[1])
        place = (first_set // 2) * (4 * s8) + (first_set % 2) * s8 + second_set
        at = iota((2 * half, count), 0)
        pair = split(ref[...])
        picked = []
        for shift in (0, 2 * s8):
            oh = one_hot(at == place + shift)
            picked.append(mm(pair[0], oh) + mm(pair[1], oh))
        real = picked[0][0:1] - picked[1][1:2]
        imag = picked[0][1:2] + picked[1][0:1]
        mine = section == target
        result[target] = [jnp.where(mine, real, 0.0), jnp.where(mine, imag, 0.0)]
    each = out_ref.shape[0] // section_count
    for target in range(section_count):
        pair = jnp.concatenate(result[target], 0)
        for r in range(each):
            out_ref[target * each + r] = pair


def local(bitstrings, boundary, stem_tensor, probe_vectors, inbound_permutations):
    rows, s8, width = stem_tensor.shape[2:]
    micro, batch, qubits = bitstrings.shape[1:]
    count = micro * batch
    section_count = lax.axis_size("a") * lax.axis_size("b")
    z_count = lax.axis_size("z")
    stem_count = z_count * lax.axis_size("c")
    assert section_count == 4 and s8 == 2 * section_count
    half = s8 * s8
    sds = jax.ShapeDtypeStruct
    vmem = pl.BlockSpec(memory_space=pltpu.VMEM)
    smem = pl.BlockSpec(memory_space=pltpu.SMEM)
    hbm = pl.BlockSpec(memory_space=pltpu.HBM)
    chunks = rows // CHUNK
    buffers = min(4, chunks)

    def call(body, limit, **kwargs):
        params = pltpu.CompilerParams(vmem_limit_bytes=limit * 2**20)
        return pl.pallas_call(body, compiler_params=params, **kwargs)

    blocks, amp0, own_set, hot, *held = call(
        functools.partial(first_body, buffers),
        8,
        out_shape=[
            sds((2 * stem_count, 2 * s8, rows), F32),
            sds((8, 2 * half), F32),
            sds((8, count), F32),
            pltpu.VMEM((width, width), BF16),
        ]
        + [pltpu.VMEM((2, rows // buffers, s8, width), F32)] * buffers,
        in_specs=[hbm] * 4 + [vmem],
        out_specs=[vmem] * (4 + buffers),
        scratch_shapes=[
            pltpu.SMEM((2, width), F32),
            pltpu.SMEM((section_count, width), jnp.int32),
            pltpu.VMEM((1, 2, width), F32),
            pltpu.VMEM((section_count, width), jnp.int32),
            pltpu.SemaphoreType.DMA((4,)),
            pltpu.SemaphoreType.DMA((chunks,)),
            pltpu.VMEM((2 * s8, width), F32),
            pltpu.VMEM((CHUNK * s8, 256), F32),
            pltpu.VMEM((2 * s8, rows * s8), F32),
        ],
        name="stage_a",
    )(boundary, inbound_permutations, stem_tensor, probe_vectors, bitstrings[0].transpose(2, 0, 1))
    recv = lax.all_to_all(blocks, ("b", "z", "c"), 0, 0, tiled=True)

    pay_rows = z_count * 4 * s8 + 2 * s8 + ROW_TILE
    pay = (section_count, pay_rows, rows)
    keep, send, amp1 = call(
        functools.partial(second_body, buffers),
        12,
        out_shape=[sds(pay, F32), sds(pay, F32), sds((8, 2 * half), F32)],
        in_specs=[vmem] * (4 + buffers),
        out_specs=[vmem, vmem, vmem],
        scratch_shapes=[
            pltpu.VMEM((2, 4 * half, rows * s8), BF16),
            pltpu.VMEM((4 * half, width), F32),
            pltpu.VMEM((2, 8 * s8, width), BF16),
            pltpu.VMEM((4 * s8, rows * s8), F32),
        ],
        name="stage_b",
    )(*held, recv, hot, probe_vectors, own_set)
    other = lax.ppermute(send, "c", [(0, 1), (1, 0)])
    packed = call(
        pack_body, 4, out_shape=sds(pay, F32), in_specs=[vmem, vmem], out_specs=vmem, name="pack"
    )(keep, other)
    got = lax.all_to_all(packed, ("a", "b"), 0, 0, tiled=True)
    u_parts = got[1, : z_count * 4 * s8].reshape(z_count, 4 * s8, rows)
    u_recv = lax.all_to_all(u_parts, "z", 0, 0, tiled=True)

    contrib = call(
        functools.partial(final_body, s8),
        8,
        out_shape=sds((section_count * stem_count, 2, count), F32),
        in_specs=[vmem] * 4,
        out_specs=vmem,
        scratch_shapes=[pltpu.VMEM((4 * s8, rows * s8), F32)],
        name="final",
    )(u_recv, got, amp0, amp1)
    arrived = lax.all_to_all(contrib, ("a", "b", "z", "c"), 0, 0, tiled=True)
    return jnp.sum(arrived, 0).reshape(1, 2, micro, batch)


def solution(mesh):
    sections, stems = (mesh.shape[name] for name in ("section", "stem"))
    devices = mesh.devices.reshape(sections // 2, 2, stems // 2, 2)
    fine = Mesh(devices, ("a", "b", "z", "c"))
    return jax.shard_map(
        local,
        mesh=fine,
        in_specs=(
            P(("a", "b")),
            P(),
            P(("a", "b"), None, ("z", "c")),
            P(("a", "b")),
            P(),
        ),
        out_specs=P(("a", "b")),
        check_vma=False,
    )
```

```python
import functools

import jax
import jax.numpy as jnp
from jax import lax
from jax.experimental import pallas as pl
from jax.experimental.pallas import tpu as pltpu
from jax.sharding import Mesh
from jax.sharding import PartitionSpec as P


F32 = jnp.float32
BF16 = jnp.bfloat16
NT = (((1,), (1,)), ((), ()))
CHUNK = 32
TILE = 256
ROW_TILE = 8


def split(x):
    high = x.astype(BF16)
    return high, (x - high.astype(F32)).astype(BF16)


def mm(a, b):
    return jnp.dot(a, b, preferred_element_type=F32)


def mm_nt(a, b):
    return lax.dot_general(a, b, NT, preferred_element_type=F32)


def iota(shape, dim):
    return lax.broadcasted_iota(jnp.int32, shape, dim)


def one_hot(cond):
    return jnp.where(cond, 1.0, 0.0).astype(BF16)


def repeat_matrix(rows, settings):
    shape = (rows, rows * settings)
    return one_hot(iota(shape, 1) // settings == iota(shape, 0))


def position():
    section = lax.axis_index("a") * lax.axis_size("b") + lax.axis_index("b")
    core = lax.axis_index("c")
    rank = lax.axis_index("z") * lax.axis_size("c") + core
    return section, rank, core


def chunk_copy(stem_hbm, bufs, sem, b, i):
    held = bufs[b].shape[1]
    source = stem_hbm.at[0, :, pl.ds(b * held + i * CHUNK, CHUNK)]
    slot = sem.at[b * (held // CHUNK) + i]
    return pltpu.make_async_copy(source, bufs[b].at[:, pl.ds(i * CHUNK, CHUNK)], slot)


def permuted_tiles(parts, hot_ref, store):
    count = parts.shape[0] // 2
    for i in range(0, hot_ref.shape[1], TILE):
        total = mm(parts, hot_ref[:, i : i + TILE])
        store(i, total[:count] + total[count:])


def probe_amplitudes(probe, vectors):
    ones = jnp.ones((8, 128), BF16)
    sums = [jnp.zeros((vectors.shape[0], 128), F32)] * 2
    for j in range(0, vectors.shape[1], 128):
        part = vectors[:, j : j + 128]
        sums = [s + part * probe[p : p + 1, j : j + 128] for p, s in enumerate(sums)]
    out = []
    for s in sums:
        hi, lo = split(s)
        out.append((mm_nt(ones, hi) + mm_nt(ones, lo))[0:1])
    return jnp.concatenate(out, 0)


def first_body(buffers, boundary_hbm, perm_hbm, stem_hbm, probe_hbm, bits_hbm, block_out, fwd_ref, set_out, hot_out, *rest):
    bufs = rest[:buffers]
    boundary_smem, perm_smem, probe_ref, perm_ref, bits_ref, small, sem, part_ref, back_ref = rest[buffers:]
    section, rank, core = position()
    held, s8, width = bufs[0].shape[1:]
    rows = held * buffers
    per = held // CHUNK
    lanes = CHUNK * s8
    stem_count = block_out.shape[0] // 2
    target = (1 - lax.axis_index("b")) * stem_count
    pairs = [
        (perm_hbm, perm_ref),
        (boundary_hbm, boundary_smem),
        (perm_hbm, perm_smem),
        (probe_hbm, probe_ref),
        (bits_hbm, bits_ref),
    ]
    little = [pltpu.make_async_copy(a, b, small.at[i]) for i, (a, b) in enumerate(pairs)]
    for copy in little:
        copy.start()
    large = [chunk_copy(stem_hbm, bufs, sem, b, i) for b in range(buffers) for i in range(per)]
    large[0].start()
    for copy in little:
        copy.wait()
    for copy in large[1:]:
        copy.start()
    settings = bits_ref[0]
    for q in range(1, bits_ref.shape[0]):
        settings += jnp.left_shift(bits_ref[q], q)
    line = jnp.concatenate([settings[i : i + 1] for i in range(settings.shape[0])], 1)
    set_out[...] = jnp.broadcast_to(line.astype(F32), set_out.shape)

    @pl.when(section <= 1)
    def _():
        wanted = perm_ref[pl.ds(section + 1, 1)]
        parts = [wanted[:, d * rows : (d + 1) * rows] for d in range(stem_count)]
        kept_first = [jnp.concatenate(parts[c::2] + parts[1 - c :: 2], 1) for c in (0, 1)]
        swapped = jnp.where(core == 0, kept_first[0], kept_first[1])
        perm_ref[0:1] = jnp.where(section == 1, swapped, wanted)

        def place(i, carry):
            at = pl.ds(pl.multiple_of(i * TILE, TILE), TILE)
            row = perm_ref[0:1, at]
            for j in range(0, width, TILE):
                hot_out[j : j + TILE, at] = one_hot(iota((TILE, TILE), 0) + j == row)
            return carry

        lax.fori_loop(0, width // TILE, place, 0)

    @pl.when(section == 2)
    def _():
        def place(i, carry):
            at = pl.ds(pl.multiple_of(i * 128, 128), 128)
            wanted = jnp.broadcast_to(perm_ref[3:4, at], (128, 128)).astype(F32).T
            for j in range(0, width, 128):
                place_at = (iota((128, 128), 1) + j).astype(F32)
                hot_out[at, j : j + 128] = one_hot(place_at == wanted)
            return carry

        lax.fori_loop(0, width // 128, place, 0)

    @pl.when((section == 1) | (section == 2))
    def _():
        for b in range(buffers):
            for i in range(per):
                chunk_copy(stem_hbm, bufs, sem, b, i).wait()

    @pl.when(section == 0)
    def _():
        fwd_ref[...] = jnp.zeros(fwd_ref.shape, F32)
        piece = min(width, 1024)

        def chunk(b, c, carry):
            chunk_copy(stem_hbm, bufs, sem, b, c).wait()
            for j in range(0, width, piece):
                at = slice(j, j + piece)

                def one(i, sums):
                    k = c * CHUNK + i
                    source = perm_smem[0, rank * rows + b * held + k]
                    b_re, b_im = boundary_smem[0, source], boundary_smem[1, source]
                    t_re, t_im = bufs[b][0, k, :, at], bufs[b][1, k, :, at]
                    return sums[0] + (b_re * t_re - b_im * t_im), sums[1] + (b_re * t_im + b_im * t_re)

                start = fwd_ref[0:s8, at], fwd_ref[s8:, at]
                done = lax.fori_loop(0, CHUNK, one, start, unroll=4)
                fwd_ref[0:s8, at], fwd_ref[s8:, at] = done
            return carry

        for b in range(buffers):
            lax.fori_loop(0, per, functools.partial(chunk, b), 0)
        full = fwd_ref[...]

        def store(i, moved):
            if rows <= TILE:
                for o in range(0, TILE, rows):
                    block_out[target + (i + o) // rows] = moved[:, o : o + rows]
            else:
                block_out[target + i // rows, :, i % rows : i % rows + TILE] = moved

        permuted_tiles(jnp.concatenate(split(full), 0), hot_out, store)

    @pl.when(section == 3)
    def _():
        ones = jnp.ones((s8, 128), BF16)
        quarters = 4
        span = width // 128 // quarters

        def chunk(b, c, carry):
            chunk_copy(stem_hbm, bufs, sem, b, c).wait()
            for q in range(quarters):
                tiles = [slice(128 * t, 128 * t + 128) for t in range(q * span, (q + 1) * span)]
                p_re = [jnp.broadcast_to(probe_ref[0, 0:1, t], (s8, 128)) for t in tiles]
                p_im = [jnp.broadcast_to(probe_ref[0, 1:2, t], (s8, 128)) for t in tiles]

                def one(i, carry):
                    k = c * CHUNK + i
                    re, im = None, None
                    for n, t in enumerate(tiles):
                        t_re, t_im = bufs[b][0, k, :, t], bufs[b][1, k, :, t]
                        r = t_re * p_re[n] - t_im * p_im[n]
                        m = t_re * p_im[n] + t_im * p_re[n]
                        re, im = (r, m) if re is None else (re + r, im + m)
                    at = pl.ds(pl.multiple_of(i * s8, s8), s8)
                    if q == 0:
                        part_ref[at, 0:128], part_ref[at, 128:] = re, im
                    else:
                        part_ref[at, 0:128] += re
                        part_ref[at, 128:] += im
                    return carry

                lax.fori_loop(0, CHUNK, one, 0, unroll=8)
            hi, lo = split(part_ref[...])
            at = pl.ds(pl.multiple_of((b * per + c) * lanes, lanes), lanes)
            for plane in range(2):
                side = slice(128 * plane, 128 * plane + 128)
                back_ref[s8 * plane : s8 * plane + s8, at] = mm_nt(ones, hi[:, side]) + mm_nt(ones, lo[:, side])
            return carry

        for b in range(buffers):
            lax.fori_loop(0, per, functools.partial(chunk, b), 0)
        group = min(rows, 128)
        rep = repeat_matrix(group, s8)
        shape = (2 * s8, group * s8)
        pick = (iota(shape, 1) % s8) == (iota(shape, 0) % s8)
        for start in range(0, rows, group):
            spread = jnp.where(pick, back_ref[:, start * s8 : (start + group) * s8], 0.0)
            hi, lo = split(spread)
            out = mm_nt(hi, rep) + mm_nt(lo, rep)
            for d in range(stem_count):
                block_out[target + d, :, start : start + group] = out


def second_body(buffers, *refs):
    bufs = refs[:buffers]
    recv_ref, hot_ref, probe_ref, set_ref, fwd_ref, keep_out, send_out, amp_out = refs[buffers : buffers + 8]
    lhs_ref, acc_ref, back_lhs_ref, back_ref = refs[buffers + 8 :]
    section, _, _ = position()
    held, s8, width = bufs[0].shape[1:]
    rows = held * buffers
    count = rows // CHUNK
    per = held // CHUNK
    lanes = CHUNK * s8
    half = s8 * s8
    stem_count = recv_ref.shape[0] // 2
    body = 4 * s8 * (stem_count // 2)
    source = (1 - lax.axis_index("b")) * stem_count
    group = min(rows, 128)
    batch = set_ref.shape[1]

    for q in range(keep_out.shape[0]):
        for i, at in enumerate(range(0, batch, rows)):
            n = min(rows, batch - at)
            keep_out[q, body + 2 * s8 + i : body + 2 * s8 + i + 1, 0:n] = set_ref[0:1, at : at + n]

    @pl.when(section == 0)
    def _():
        gap = jnp.zeros((s8, width), F32)
        spaced = jnp.concatenate([fwd_ref[:s8], gap, fwd_ref[s8:], gap], 0)
        amp_out[0:2, 0 : 4 * s8] = probe_amplitudes(probe_ref[0], spaced)

    @pl.when(section == 1)
    def _():
        acc_ref[...] = jnp.zeros(acc_ref.shape, F32)
        state = recv_ref[source]
        for d in range(1, stem_count):
            state += recv_ref[source + d]
        rep = repeat_matrix(group, s8)
        mask_shape = (2 * s8, group * s8)
        pick = (iota(mask_shape, 1) % s8) == (iota(mask_shape, 0) % s8)
        upper = iota(mask_shape, 0) < s8
        for start in range(0, rows, group):
            hi, lo = split(state[:, start : start + group])
            wide = mm(jnp.concatenate([hi, lo], 0), rep)
            at = pl.ds(start * s8, group * s8)
            for level in range(2):
                for quarter in range(s8 // 2):
                    base = level * 2 * s8 + 2 * quarter
                    built = []
                    for plane in range(2):
                        r = base + plane * s8
                        value = jnp.where(upper, wide[r : r + 1], wide[r + 1 : r + 2])
                        built.append(jnp.where(pick, value, 0.0))
                    top = level * 2 * half + quarter * 4 * s8
                    lo_rows = pl.ds(top, 2 * s8)
                    hi_rows = pl.ds(top + 2 * s8, 2 * s8)
                    lhs_ref[0, lo_rows, at] = built[0].astype(BF16)
                    lhs_ref[0, hi_rows, at] = built[1].astype(BF16)
                    lhs_ref[1, lo_rows, at] = (-built[1]).astype(BF16)
                    lhs_ref[1, hi_rows, at] = built[0].astype(BF16)

        for c in range(count):
            at = slice(c * lanes, (c + 1) * lanes)
            ks = slice(c % per * CHUNK, (c % per + 1) * CHUNK)
            for j in range(0, width, 2 * TILE):
                cols = slice(j, j + 2 * TILE)
                total = acc_ref[:, cols]
                extra = jnp.zeros((2 * half, 2 * TILE), F32)
                for plane in range(2):
                    hi, lo = split(bufs[c // per][plane, ks, :, cols].reshape(lanes, 2 * TILE))
                    e = lhs_ref[plane, :, at]
                    total += mm(e, hi)
                    extra += mm(e[: 2 * half], lo)
                acc_ref[0 : 2 * half, cols] = total[: 2 * half] + extra
                acc_ref[2 * half :, cols] = total[2 * half :]
        full = acc_ref[0 : 2 * half] + acc_ref[2 * half :]
        amp_out[0:2] = probe_amplitudes(probe_ref[0], full)

        def store(i, moved):
            n = min(rows, TILE)
            for o in range(0, TILE, n):
                slot, lane = divmod(i + o, rows)
                z, ref = slot % (stem_count // 2), (keep_out, send_out)[slot // (stem_count // 2)]
                for q in range(s8 // 2):
                    piece = moved[q * 4 * s8 : (q + 1) * 4 * s8, o : o + n]
                    ref[q, z * 4 * s8 : (z + 1) * 4 * s8, lane : lane + n] = piece

        permuted_tiles(jnp.concatenate(split(full), 0), hot_ref, store)

    @pl.when(section == 2)
    def _():
        zero = jnp.zeros((s8 - 1, width), F32)
        pieces = [split(recv_ref[source + d]) for d in range(stem_count)]
        parts = jnp.concatenate([jnp.concatenate([p[i] for p in pieces], 1) for i in (0, 1)], 0)
        moved = []
        permuted_tiles(parts, hot_ref, lambda i, x: moved.append(x))
        moved = jnp.concatenate(moved, 1)
        real = jnp.concatenate([moved[:s8], probe_ref[0, 0:1], zero], 0)
        imag = jnp.concatenate([moved[s8:], probe_ref[0, 1:2], zero], 0)
        count = 4 * s8
        blank = jnp.zeros((128 - 2 * count, width), BF16)
        for plane, pair in enumerate([(real, imag), (-imag, real)]):
            hi, lo = split(jnp.concatenate(pair, 0))
            back_lhs_ref[plane, 0] = jnp.concatenate([hi, lo, blank], 0)
            back_lhs_ref[plane, 1] = jnp.concatenate([hi, jnp.zeros(lo.shape, BF16), blank], 0)
        for b in range(buffers):
            total = jnp.zeros((held * s8, 128), F32)
            for plane in range(2):
                for level, part in enumerate(split(bufs[b][plane].reshape(held * s8, width))):
                    total += mm_nt(part, back_lhs_ref[plane, level])
            turned = total.T
            at = slice(b * held * s8, (b + 1) * held * s8)
            back_ref[:, at] = turned[:count] + turned[count : 2 * count]
        for i in range(s8):
            at = slice(i * rows, (i + 1) * rows)
            for q in range(keep_out.shape[0]):
                for plane in range(2):
                    row = 2 * s8 * (i) + plane * s8
                    keep_out[q, row : row + s8, :] = back_ref[2 * s8 * plane : 2 * s8 * plane + s8, at]
                    row = body + 2 * i + plane
                    src = 2 * s8 * plane + s8
                    keep_out[q, row : row + 1, :] = back_ref[src : src + 1, at]


def pack_body(keep_ref, recv_ref, out_ref):
    section, _, _ = position()

    @pl.when(section == 1)
    def _():
        out_ref[...] = keep_ref[...] + recv_ref[...]
        tail = keep_ref.shape[1] - ROW_TILE
        out_ref[:, tail:] = keep_ref[:, tail:]

    @pl.when(section != 1)
    def _():
        out_ref[...] = keep_ref[...]


def final_body(settings, u_ref, got_ref, amp_ref, out_ref, x_ref):
    s8 = settings
    section, _, _ = position()
    half = s8 * s8
    section_count = got_ref.shape[0]
    rows = u_ref.shape[2]
    count = out_ref.shape[2]
    body = u_ref.shape[0] * 4 * s8
    u = u_ref[0]
    for z in range(1, u_ref.shape[0]):
        u += u_ref[z]
    x_ref[...] = jnp.zeros(x_ref.shape, F32)
    for i in range(s8):
        at = slice(i * rows, (i + 1) * rows)
        for plane in range(2):
            row = 2 * s8 * i + plane * s8
            x_ref[2 * s8 * plane : 2 * s8 * plane + s8, at] = got_ref[2, row : row + s8]
            row = body + 2 * i + plane
            to = 2 * s8 * plane + s8
            x_ref[to : to + 1, at] = got_ref[2, row : row + 1]
    group = min(rows, 128)
    rep = repeat_matrix(group, s8)
    shape = (s8, group * s8)
    pick = (iota(shape, 1) % s8) == iota(shape, 0)
    table = jnp.zeros((4 * s8, 4 * half), F32)
    for start in range(0, rows, group):
        hi, lo = split(u[:, start : start + group])
        wide = mm(jnp.concatenate([hi, lo], 0), rep)
        spread = []
        for level in range(2):
            tiles = [
                jnp.where(pick, wide[r : r + 1], 0.0)
                for r in range(level * 4 * s8, (level + 1) * 4 * s8)
            ]
            spread.append(jnp.concatenate(tiles, 0).astype(BF16))
        x_hi, x_lo = split(x_ref[:, start * s8 : (start + group) * s8])
        both = mm_nt(jnp.concatenate([x_hi, x_lo], 0), spread[0])
        table += both[: 4 * s8] + both[4 * s8 :] + mm_nt(x_hi, spread[1])
    per = 2 * s8 * s8
    re_u, im_u = table[:, :per], table[:, per:]
    c_re = re_u[: 2 * s8] - im_u[2 * s8 :]
    c_im = re_u[2 * s8 :] + im_u[: 2 * s8]
    top = body + 2 * s8
    s = []
    for i in range(section_count):
        pieces = [
            got_ref[i, top + n : top + n + 1, 0 : min(rows, count - at)]
            for n, at in enumerate(range(0, count, rows))
        ]
        s.append(jnp.concatenate(pieces, 1).astype(jnp.int32))
    code = ((s[0] % 2) * s8 + s[1]) * s8 + s[2]
    sel = one_hot((iota((per, count), 0) == code) & (s[0] // 2 == section))
    parts = split(jnp.concatenate([c_re, c_im], 0))
    chosen = mm(parts[0], sel) + mm(parts[1], sel)
    match = iota((s8, count), 0) == s[3]
    result = [[None, None] for _ in range(section_count)]
    for plane in range(2):
        top = plane * 2 * s8
        result[3][plane] = jnp.sum(jnp.where(match, chosen[top : top + s8], 0.0), 0, keepdims=True)
        result[2][plane] = chosen[top + s8 : top + s8 + 1]
    lead = jnp.where(section == 0, 0, s[0])
    ending = jnp.where(section == 0, s[0], s[1])
    place = (lead // 2) * (4 * s8) + (lead % 2) * s8 + ending
    at = iota((2 * half, count), 0)
    valid = iota((8, 2 * half), 1) < jnp.where(section == 0, 4 * s8, 2 * half)
    pair = split(jnp.where(valid & (section < 2), amp_ref[...], 0.0))
    picked = []
    for shift in (0, 2 * s8):
        oh = one_hot(at == place + shift)
        picked.append(mm(pair[0], oh) + mm(pair[1], oh))
    real = picked[0][0:1] - picked[1][1:2]
    imag = picked[0][1:2] + picked[1][0:1]
    for target in (0, 1):
        mine = section == target
        result[target] = [jnp.where(mine, real, 0.0), jnp.where(mine, imag, 0.0)]
    each = out_ref.shape[0] // section_count
    for target in range(section_count):
        pair = jnp.concatenate(result[target], 0)
        for r in range(each):
            out_ref[target * each + r] = pair


def local(bitstrings, boundary, stem_tensor, probe_vectors, inbound_permutations):
    rows, s8, width = stem_tensor.shape[2:]
    micro, batch, qubits = bitstrings.shape[1:]
    count = micro * batch
    section_count = lax.axis_size("a") * lax.axis_size("b")
    z_count = lax.axis_size("z")
    stem_count = z_count * lax.axis_size("c")
    assert section_count == 4 and s8 == 2 * section_count
    half = s8 * s8
    sds = jax.ShapeDtypeStruct
    vmem = pl.BlockSpec(memory_space=pltpu.VMEM)
    smem = pl.BlockSpec(memory_space=pltpu.SMEM)
    hbm = pl.BlockSpec(memory_space=pltpu.HBM)
    operands = boundary, inbound_permutations, stem_tensor, probe_vectors, bitstrings[0].transpose(2, 0, 1)
    chunks = rows // CHUNK
    buffers = min(4, chunks)

    def call(body, limit, **kwargs):
        params = pltpu.CompilerParams(vmem_limit_bytes=limit * 2**20)
        return pl.pallas_call(body, compiler_params=params, **kwargs)

    blocks, firsts, own_set, hot, *held = call(
        functools.partial(first_body, buffers),
        8,
        out_shape=[
            sds((2 * stem_count, 2 * s8, rows), F32),
            pltpu.VMEM((2 * s8, width), F32),
            sds((8, count), F32),
            pltpu.VMEM((width, width), BF16),
        ]
        + [pltpu.VMEM((2, rows // buffers, s8, width), F32)] * buffers,
        in_specs=[hbm] * 5,
        out_specs=[vmem] * (4 + buffers),
        scratch_shapes=[
            pltpu.SMEM((2, width), F32),
            pltpu.SMEM((section_count, width), jnp.int32),
            pltpu.VMEM((1, 2, width), F32),
            pltpu.VMEM((section_count, width), jnp.int32),
            pltpu.VMEM((qubits, micro, batch), jnp.int32),
            pltpu.SemaphoreType.DMA((5,)),
            pltpu.SemaphoreType.DMA((chunks,)),
            pltpu.VMEM((CHUNK * s8, 256), F32),
            pltpu.VMEM((2 * s8, rows * s8), F32),
        ],
        name="stage_a",
    )(*(pltpu.with_memory_space_constraint(x, pltpu.HBM) for x in operands))
    recv = lax.all_to_all(blocks, ("b", "z", "c"), 0, 0, tiled=True)

    pay_rows = z_count * 4 * s8 + 2 * s8 + ROW_TILE
    pay = (section_count, pay_rows, rows)
    keep, send, amps = call(
        functools.partial(second_body, buffers),
        12,
        out_shape=[sds(pay, F32), sds(pay, F32), sds((8, 2 * half), F32)],
        in_specs=[vmem] * (5 + buffers),
        out_specs=[vmem, vmem, vmem],
        scratch_shapes=[
            pltpu.VMEM((2, 4 * half, rows * s8), BF16),
            pltpu.VMEM((4 * half, width), F32),
            pltpu.VMEM((2, 2, 128, width), BF16),
            pltpu.VMEM((4 * s8, rows * s8), F32),
        ],
        name="stage_b",
    )(*held, recv, hot, probe_vectors, own_set, firsts)
    other = lax.ppermute(send, "c", [(0, 1), (1, 0)])
    packed = call(
        pack_body, 4, out_shape=sds(pay, F32), in_specs=[vmem, vmem], out_specs=vmem, name="pack"
    )(keep, other)
    got = lax.all_to_all(packed, ("a", "b"), 0, 0, tiled=True)
    u_parts = got[1, : z_count * 4 * s8].reshape(z_count, 4 * s8, rows)
    u_recv = lax.all_to_all(u_parts, "z", 0, 0, tiled=True)

    contrib = call(
        functools.partial(final_body, s8),
        8,
        out_shape=sds((section_count * stem_count, 2, count), F32),
        in_specs=[vmem] * 3,
        out_specs=vmem,
        scratch_shapes=[pltpu.VMEM((4 * s8, rows * s8), F32)],
        name="final",
    )(u_recv, got, amps)
    arrived = lax.all_to_all(contrib, ("a", "b", "z", "c"), 0, 0, tiled=True)
    return jnp.sum(arrived, 0).reshape(1, 2, micro, batch)


def solution(mesh):
    sections, stems = (mesh.shape[name] for name in ("section", "stem"))
    devices = mesh.devices.reshape(sections // 2, 2, stems // 2, 2)
    fine = Mesh(devices, ("a", "b", "z", "c"))
    return jax.shard_map(
        local,
        mesh=fine,
        in_specs=(
            P(("a", "b")),
            P(),
            P(("a", "b"), None, ("z", "c")),
            P(("a", "b")),
            P(),
        ),
        out_specs=P(("a", "b")),
        check_vma=False,
    )
```

```python
import functools

import jax
import jax.numpy as jnp
from jax import lax
from jax.experimental import pallas as pl
from jax.experimental.pallas import tpu as pltpu
from jax.sharding import Mesh
from jax.sharding import PartitionSpec as P


F32 = jnp.float32
BF16 = jnp.bfloat16
NT = (((1,), (1,)), ((), ()))
CHUNK = 32
TILE = 256
ROW_TILE = 8


def split(x):
    high = x.astype(BF16)
    return high, (x - high.astype(F32)).astype(BF16)


def mm(a, b):
    return jnp.dot(a, b, preferred_element_type=F32)


def mm_nt(a, b):
    return lax.dot_general(a, b, NT, preferred_element_type=F32)


def iota(shape, dim):
    return lax.broadcasted_iota(jnp.int32, shape, dim)


def one_hot(cond):
    return jnp.where(cond, 1.0, 0.0).astype(BF16)


def repeat_matrix(rows, settings):
    shape = (rows, rows * settings)
    return one_hot(iota(shape, 1) // settings == iota(shape, 0))


def position():
    section = lax.axis_index("a") * lax.axis_size("b") + lax.axis_index("b")
    core = lax.axis_index("c")
    rank = lax.axis_index("z") * lax.axis_size("c") + core
    return section, rank, core


def chunk_copy(stem_hbm, bufs, sem, b, i):
    held = bufs[b].shape[1]
    source = stem_hbm.at[0, :, pl.ds(b * held + i * CHUNK, CHUNK)]
    slot = sem.at[b * (held // CHUNK) + i]
    return pltpu.make_async_copy(source, bufs[b].at[:, pl.ds(i * CHUNK, CHUNK)], slot)


def permuted_tiles(parts, hot_ref, store):
    count = parts.shape[0] // 2
    for i in range(0, hot_ref.shape[1], TILE):
        total = mm(parts, hot_ref[:, i : i + TILE])
        store(i, total[:count] + total[count:])


def gathered_tiles(source_ref, order_ref, store):
    count, width = 2 * ROW_TILE, source_ref.shape[1]
    for i in range(0, width, 128):
        index = jnp.broadcast_to(order_ref[0:1, i : i + 128], (ROW_TILE, 128))
        lane, tile = index % 128, index // 128
        pieces = []
        for r in range(0, count, ROW_TILE):
            piece = jnp.zeros((ROW_TILE, 128), F32)
            for t in range(width // 128):
                part = source_ref[r : r + ROW_TILE, 128 * t : 128 * t + 128]
                got = jnp.take_along_axis(part, lane, axis=1, mode="promise_in_bounds")
                piece = jnp.where(tile == t, got, piece)
            pieces.append(piece)
        store(i, jnp.concatenate(pieces, 0))


def probe_amplitudes(probe, vectors):
    ones = jnp.ones((8, 128), BF16)
    sums = [jnp.zeros((vectors.shape[0], 128), F32)] * 2
    for j in range(0, vectors.shape[1], 128):
        part = vectors[:, j : j + 128]
        sums = [s + part * probe[p : p + 1, j : j + 128] for p, s in enumerate(sums)]
    out = []
    for s in sums:
        hi, lo = split(s)
        out.append((mm_nt(ones, hi) + mm_nt(ones, lo))[0:1])
    return jnp.concatenate(out, 0)


def first_body(buffers, boundary_hbm, perm_hbm, stem_hbm, probe_hbm, bits_hbm, block_out, fwd_ref, set_out, back_order_out, hot_out, *rest):
    bufs = rest[:buffers]
    boundary_smem, perm_smem, probe_ref, perm_ref, bits_ref, small, sem, part_ref, back_ref = rest[buffers:]
    section, rank, core = position()
    held, s8, width = bufs[0].shape[1:]
    rows = held * buffers
    per = held // CHUNK
    lanes = CHUNK * s8
    stem_count = block_out.shape[0] // 2
    target = (1 - lax.axis_index("b")) * stem_count
    pairs = [
        (perm_hbm, perm_ref),
        (boundary_hbm, boundary_smem),
        (perm_hbm, perm_smem),
        (probe_hbm, probe_ref),
        (bits_hbm, bits_ref),
    ]
    little = [pltpu.make_async_copy(a, b, small.at[i]) for i, (a, b) in enumerate(pairs)]
    for copy in little:
        copy.start()
    large = [chunk_copy(stem_hbm, bufs, sem, b, i) for b in range(buffers) for i in range(per)]
    large[0].start()
    for copy in little:
        copy.wait()
    for copy in large[1:]:
        copy.start()
    settings = bits_ref[0]
    for q in range(1, bits_ref.shape[0]):
        settings += jnp.left_shift(bits_ref[q], q)
    line = jnp.concatenate([settings[i : i + 1] for i in range(settings.shape[0])], 1)
    set_out[...] = jnp.broadcast_to(line.astype(F32), set_out.shape)

    @pl.when(section == 0)
    def _():
        perm_ref[0:1] = perm_ref[1:2]

    @pl.when(section == 1)
    def _():
        wanted = perm_ref[2:3]
        parts = [wanted[:, d * rows : (d + 1) * rows] for d in range(stem_count)]
        kept_first = [jnp.concatenate(parts[c::2] + parts[1 - c :: 2], 1) for c in (0, 1)]
        perm_ref[0:1] = jnp.where(core == 0, kept_first[0], kept_first[1])

        def place(i, carry):
            at = pl.ds(pl.multiple_of(i * TILE, TILE), TILE)
            row = perm_ref[0:1, at]
            for j in range(0, width, TILE):
                hot_out[j : j + TILE, at] = one_hot(iota((TILE, TILE), 0) + j == row)
            return carry

        lax.fori_loop(0, width // TILE, place, 0)

    @pl.when(section == 2)
    def _():
        def place(i, carry):
            at = pl.ds(pl.multiple_of(i * 128, 128), 128)
            wanted = jnp.broadcast_to(perm_ref[3:4, at], (128, 128)).astype(F32).T
            for j in range(0, width, 128):
                place_at = (iota((128, 128), 1) + j).astype(F32)
                hot_out[at, j : j + 128] = one_hot(place_at == wanted)
            return carry

        lax.fori_loop(0, width // 128, place, 0)
        number = iota((16, width), 1)
        digits = jnp.where(iota((16, width), 0) == 0, number // 128, number % 128)
        digits = digits.astype(F32).astype(BF16)
        for j in range(0, width, TILE):
            found = mm(digits, hot_out[:, j : j + TILE])
            line = (found[0:1] * 128.0 + found[1:2]).astype(jnp.int32)
            back_order_out[:, j : j + TILE] = jnp.broadcast_to(line, (ROW_TILE, TILE))

    @pl.when((section == 1) | (section == 2))
    def _():
        for b in range(buffers):
            for i in range(per):
                chunk_copy(stem_hbm, bufs, sem, b, i).wait()

    @pl.when(section == 0)
    def _():
        fwd_ref[...] = jnp.zeros(fwd_ref.shape, F32)
        piece = min(width, 1024)

        def chunk(b, c, carry):
            chunk_copy(stem_hbm, bufs, sem, b, c).wait()
            for j in range(0, width, piece):
                at = slice(j, j + piece)

                def one(i, sums):
                    k = c * CHUNK + i
                    source = perm_smem[0, rank * rows + b * held + k]
                    b_re, b_im = boundary_smem[0, source], boundary_smem[1, source]
                    t_re, t_im = bufs[b][0, k, :, at], bufs[b][1, k, :, at]
                    return sums[0] + (b_re * t_re - b_im * t_im), sums[1] + (b_re * t_im + b_im * t_re)

                start = fwd_ref[0:s8, at], fwd_ref[s8:, at]
                done = lax.fori_loop(0, CHUNK, one, start, unroll=4)
                fwd_ref[0:s8, at], fwd_ref[s8:, at] = done
            return carry

        for b in range(buffers):
            lax.fori_loop(0, per, functools.partial(chunk, b), 0)
        def store(i, moved):
            n = min(rows, 128)
            for o in range(0, 128, n):
                dest, lane = divmod(i + o, rows)
                block_out[target + dest, :, lane : lane + n] = moved[:, o : o + n]

        gathered_tiles(fwd_ref, perm_ref, store)

    @pl.when(section == 3)
    def _():
        ones = jnp.ones((s8, 128), BF16)
        quarters = 4
        span = width // 128 // quarters

        def chunk(b, c, carry):
            chunk_copy(stem_hbm, bufs, sem, b, c).wait()
            for q in range(quarters):
                tiles = [slice(128 * t, 128 * t + 128) for t in range(q * span, (q + 1) * span)]
                p_re = [jnp.broadcast_to(probe_ref[0, 0:1, t], (s8, 128)) for t in tiles]
                p_im = [jnp.broadcast_to(probe_ref[0, 1:2, t], (s8, 128)) for t in tiles]

                def one(i, carry):
                    k = c * CHUNK + i
                    re, im = None, None
                    for n, t in enumerate(tiles):
                        t_re, t_im = bufs[b][0, k, :, t], bufs[b][1, k, :, t]
                        r = t_re * p_re[n] - t_im * p_im[n]
                        m = t_re * p_im[n] + t_im * p_re[n]
                        re, im = (r, m) if re is None else (re + r, im + m)
                    at = pl.ds(pl.multiple_of(i * s8, s8), s8)
                    if q == 0:
                        part_ref[at, 0:128], part_ref[at, 128:] = re, im
                    else:
                        part_ref[at, 0:128] += re
                        part_ref[at, 128:] += im
                    return carry

                lax.fori_loop(0, CHUNK, one, 0, unroll=8)
            hi, lo = split(part_ref[...])
            at = pl.ds(pl.multiple_of((b * per + c) * lanes, lanes), lanes)
            for plane in range(2):
                side = slice(128 * plane, 128 * plane + 128)
                back_ref[s8 * plane : s8 * plane + s8, at] = mm_nt(ones, hi[:, side]) + mm_nt(ones, lo[:, side])
            return carry

        for b in range(buffers):
            lax.fori_loop(0, per, functools.partial(chunk, b), 0)
        group = min(rows, 128)
        rep = repeat_matrix(group, s8)
        shape = (2 * s8, group * s8)
        pick = (iota(shape, 1) % s8) == (iota(shape, 0) % s8)
        for start in range(0, rows, group):
            spread = jnp.where(pick, back_ref[:, start * s8 : (start + group) * s8], 0.0)
            hi, lo = split(spread)
            out = mm_nt(hi, rep) + mm_nt(lo, rep)
            for d in range(stem_count):
                block_out[target + d, :, start : start + group] = out


def second_body(buffers, *refs):
    bufs = refs[:buffers]
    recv_ref, hot_ref, probe_ref, set_ref, fwd_ref, order_ref, keep_out, send_out, amp_out = refs[buffers : buffers + 9]
    lhs_ref, acc_ref, back_lhs_ref, back_ref = refs[buffers + 9 :]
    section, _, _ = position()
    held, s8, width = bufs[0].shape[1:]
    rows = held * buffers
    count = rows // CHUNK
    per = held // CHUNK
    lanes = CHUNK * s8
    half = s8 * s8
    stem_count = recv_ref.shape[0] // 2
    body = 4 * s8 * (stem_count // 2)
    source = (1 - lax.axis_index("b")) * stem_count
    group = min(rows, 128)
    batch = set_ref.shape[1]

    for q in range(keep_out.shape[0]):
        for i, at in enumerate(range(0, batch, rows)):
            n = min(rows, batch - at)
            keep_out[q, body + 2 * s8 + i : body + 2 * s8 + i + 1, 0:n] = set_ref[0:1, at : at + n]

    @pl.when(section == 0)
    def _():
        gap = jnp.zeros((s8, width), F32)
        spaced = jnp.concatenate([fwd_ref[:s8], gap, fwd_ref[s8:], gap], 0)
        amp_out[0:2, 0 : 4 * s8] = probe_amplitudes(probe_ref[0], spaced)

    @pl.when(section == 1)
    def _():
        acc_ref[...] = jnp.zeros(acc_ref.shape, F32)
        state = recv_ref[source]
        for d in range(1, stem_count):
            state += recv_ref[source + d]
        rep = repeat_matrix(group, s8)
        mask_shape = (2 * s8, group * s8)
        pick = (iota(mask_shape, 1) % s8) == (iota(mask_shape, 0) % s8)
        upper = iota(mask_shape, 0) < s8
        for start in range(0, rows, group):
            hi, lo = split(state[:, start : start + group])
            wide = mm(jnp.concatenate([hi, lo], 0), rep)
            at = pl.ds(start * s8, group * s8)
            for level in range(2):
                for quarter in range(s8 // 2):
                    base = level * 2 * s8 + 2 * quarter
                    built = []
                    for plane in range(2):
                        r = base + plane * s8
                        value = jnp.where(upper, wide[r : r + 1], wide[r + 1 : r + 2])
                        built.append(jnp.where(pick, value, 0.0))
                    top = level * 2 * half + quarter * 4 * s8
                    lo_rows = pl.ds(top, 2 * s8)
                    hi_rows = pl.ds(top + 2 * s8, 2 * s8)
                    lhs_ref[0, lo_rows, at] = built[0].astype(BF16)
                    lhs_ref[0, hi_rows, at] = built[1].astype(BF16)
                    lhs_ref[1, lo_rows, at] = (-built[1]).astype(BF16)
                    lhs_ref[1, hi_rows, at] = built[0].astype(BF16)

        for c in range(count):
            at = slice(c * lanes, (c + 1) * lanes)
            ks = slice(c % per * CHUNK, (c % per + 1) * CHUNK)
            for j in range(0, width, 2 * TILE):
                cols = slice(j, j + 2 * TILE)
                total = acc_ref[:, cols]
                extra = jnp.zeros((2 * half, 2 * TILE), F32)
                for plane in range(2):
                    hi, lo = split(bufs[c // per][plane, ks, :, cols].reshape(lanes, 2 * TILE))
                    e = lhs_ref[plane, :, at]
                    total += mm(e, hi)
                    extra += mm(e[: 2 * half], lo)
                acc_ref[0 : 2 * half, cols] = total[: 2 * half] + extra
                acc_ref[2 * half :, cols] = total[2 * half :]
        full = acc_ref[0 : 2 * half] + acc_ref[2 * half :]
        amp_out[0:2] = probe_amplitudes(probe_ref[0], full)

        def store(i, moved):
            n = min(rows, TILE)
            for o in range(0, TILE, n):
                slot, lane = divmod(i + o, rows)
                z, ref = slot % (stem_count // 2), (keep_out, send_out)[slot // (stem_count // 2)]
                for q in range(s8 // 2):
                    piece = moved[q * 4 * s8 : (q + 1) * 4 * s8, o : o + n]
                    ref[q, z * 4 * s8 : (z + 1) * 4 * s8, lane : lane + n] = piece

        permuted_tiles(jnp.concatenate(split(full), 0), hot_ref, store)

    @pl.when(section == 2)
    def _():
        zero = jnp.zeros((s8 - 1, width), F32)
        for d in range(stem_count):
            acc_ref[0 : 2 * s8, d * rows : (d + 1) * rows] = recv_ref[source + d]
        moved = []
        gathered_tiles(acc_ref, order_ref, lambda i, x: moved.append(x))
        moved = jnp.concatenate(moved, 1)
        real = jnp.concatenate([moved[:s8], probe_ref[0, 0:1], zero], 0)
        imag = jnp.concatenate([moved[s8:], probe_ref[0, 1:2], zero], 0)
        count = 4 * s8
        blank = jnp.zeros((128 - 2 * count, width), BF16)
        for plane, pair in enumerate([(real, imag), (-imag, real)]):
            hi, lo = split(jnp.concatenate(pair, 0))
            back_lhs_ref[plane, 0] = jnp.concatenate([hi, lo, blank], 0)
            back_lhs_ref[plane, 1] = jnp.concatenate([hi, jnp.zeros(lo.shape, BF16), blank], 0)
        for b in range(buffers):
            total = jnp.zeros((held * s8, 128), F32)
            for plane in range(2):
                for level, part in enumerate(split(bufs[b][plane].reshape(held * s8, width))):
                    total += mm_nt(part, back_lhs_ref[plane, level])
            turned = total.T
            at = slice(b * held * s8, (b + 1) * held * s8)
            back_ref[:, at] = turned[:count] + turned[count : 2 * count]
        for i in range(s8):
            at = slice(i * rows, (i + 1) * rows)
            for q in range(keep_out.shape[0]):
                for plane in range(2):
                    row = 2 * s8 * (i) + plane * s8
                    keep_out[q, row : row + s8, :] = back_ref[2 * s8 * plane : 2 * s8 * plane + s8, at]
                    row = body + 2 * i + plane
                    src = 2 * s8 * plane + s8
                    keep_out[q, row : row + 1, :] = back_ref[src : src + 1, at]


def pack_body(keep_ref, recv_ref, out_ref):
    section, _, _ = position()

    @pl.when(section == 1)
    def _():
        out_ref[...] = keep_ref[...] + recv_ref[...]
        tail = keep_ref.shape[1] - ROW_TILE
        out_ref[:, tail:] = keep_ref[:, tail:]

    @pl.when(section != 1)
    def _():
        out_ref[...] = keep_ref[...]


def final_body(settings, u_ref, got_ref, amp_ref, out_ref, x_ref):
    s8 = settings
    section, _, _ = position()
    half = s8 * s8
    section_count = got_ref.shape[0]
    rows = u_ref.shape[2]
    count = out_ref.shape[2]
    body = u_ref.shape[0] * 4 * s8
    u = u_ref[0]
    for z in range(1, u_ref.shape[0]):
        u += u_ref[z]
    x_ref[...] = jnp.zeros(x_ref.shape, F32)
    for i in range(s8):
        at = slice(i * rows, (i + 1) * rows)
        for plane in range(2):
            row = 2 * s8 * i + plane * s8
            x_ref[2 * s8 * plane : 2 * s8 * plane + s8, at] = got_ref[2, row : row + s8]
            row = body + 2 * i + plane
            to = 2 * s8 * plane + s8
            x_ref[to : to + 1, at] = got_ref[2, row : row + 1]
    group = min(rows, 128)
    rep = repeat_matrix(group, s8)
    shape = (s8, group * s8)
    pick = (iota(shape, 1) % s8) == iota(shape, 0)
    table = jnp.zeros((4 * s8, 4 * half), F32)
    for start in range(0, rows, group):
        hi, lo = split(u[:, start : start + group])
        wide = mm(jnp.concatenate([hi, lo], 0), rep)
        spread = []
        for level in range(2):
            tiles = [
                jnp.where(pick, wide[r : r + 1], 0.0)
                for r in range(level * 4 * s8, (level + 1) * 4 * s8)
            ]
            spread.append(jnp.concatenate(tiles, 0).astype(BF16))
        x_hi, x_lo = split(x_ref[:, start * s8 : (start + group) * s8])
        both = mm_nt(jnp.concatenate([x_hi, x_lo], 0), spread[0])
        table += both[: 4 * s8] + both[4 * s8 :] + mm_nt(x_hi, spread[1])
    per = 2 * s8 * s8
    re_u, im_u = table[:, :per], table[:, per:]
    c_re = re_u[: 2 * s8] - im_u[2 * s8 :]
    c_im = re_u[2 * s8 :] + im_u[: 2 * s8]
    top = body + 2 * s8
    s = []
    for i in range(section_count):
        pieces = [
            got_ref[i, top + n : top + n + 1, 0 : min(rows, count - at)]
            for n, at in enumerate(range(0, count, rows))
        ]
        s.append(jnp.concatenate(pieces, 1).astype(jnp.int32))
    code = ((s[0] % 2) * s8 + s[1]) * s8 + s[2]
    sel = one_hot((iota((per, count), 0) == code) & (s[0] // 2 == section))
    parts = split(jnp.concatenate([c_re, c_im], 0))
    chosen = mm(parts[0], sel) + mm(parts[1], sel)
    match = iota((s8, count), 0) == s[3]
    result = [[None, None] for _ in range(section_count)]
    for plane in range(2):
        top = plane * 2 * s8
        result[3][plane] = jnp.sum(jnp.where(match, chosen[top : top + s8], 0.0), 0, keepdims=True)
        result[2][plane] = chosen[top + s8 : top + s8 + 1]
    lead = jnp.where(section == 0, 0, s[0])
    ending = jnp.where(section == 0, s[0], s[1])
    place = (lead // 2) * (4 * s8) + (lead % 2) * s8 + ending
    at = iota((2 * half, count), 0)
    valid = iota((8, 2 * half), 1) < jnp.where(section == 0, 4 * s8, 2 * half)
    pair = split(jnp.where(valid & (section < 2), amp_ref[...], 0.0))
    picked = []
    for shift in (0, 2 * s8):
        oh = one_hot(at == place + shift)
        picked.append(mm(pair[0], oh) + mm(pair[1], oh))
    real = picked[0][0:1] - picked[1][1:2]
    imag = picked[0][1:2] + picked[1][0:1]
    for target in (0, 1):
        mine = section == target
        result[target] = [jnp.where(mine, real, 0.0), jnp.where(mine, imag, 0.0)]
    each = out_ref.shape[0] // section_count
    for target in range(section_count):
        pair = jnp.concatenate(result[target], 0)
        for r in range(each):
            out_ref[target * each + r] = pair


def total_body(part_ref, out_ref):
    total = part_ref[0]
    for i in range(1, part_ref.shape[0]):
        total += part_ref[i]
    micro, batch = out_ref.shape[2:]
    for m in range(micro):
        for plane in range(2):
            out_ref[0, plane, m : m + 1] = total[plane : plane + 1, m * batch : (m + 1) * batch]


def local(bitstrings, boundary, stem_tensor, probe_vectors, inbound_permutations):
    rows, s8, width = stem_tensor.shape[2:]
    micro, batch, qubits = bitstrings.shape[1:]
    count = micro * batch
    section_count = lax.axis_size("a") * lax.axis_size("b")
    z_count = lax.axis_size("z")
    stem_count = z_count * lax.axis_size("c")
    assert section_count == 4 and s8 == 2 * section_count
    half = s8 * s8
    sds = jax.ShapeDtypeStruct
    vmem = pl.BlockSpec(memory_space=pltpu.VMEM)
    smem = pl.BlockSpec(memory_space=pltpu.SMEM)
    hbm = pl.BlockSpec(memory_space=pltpu.HBM)
    operands = boundary, inbound_permutations, stem_tensor, probe_vectors, bitstrings[0].transpose(2, 0, 1)
    chunks = rows // CHUNK
    buffers = min(4, chunks)

    def call(body, limit, **kwargs):
        params = pltpu.CompilerParams(vmem_limit_bytes=limit * 2**20)
        return pl.pallas_call(body, compiler_params=params, **kwargs)

    blocks, firsts, own_set, back_order, hot, *held = call(
        functools.partial(first_body, buffers),
        8,
        out_shape=[
            sds((2 * stem_count, 2 * s8, rows), F32),
            pltpu.VMEM((2 * s8, width), F32),
            sds((8, count), F32),
            sds((ROW_TILE, width), jnp.int32),
            pltpu.VMEM((width, width), BF16),
        ]
        + [pltpu.VMEM((2, rows // buffers, s8, width), F32)] * buffers,
        in_specs=[hbm] * 5,
        out_specs=[vmem] * (5 + buffers),
        scratch_shapes=[
            pltpu.SMEM((2, width), F32),
            pltpu.SMEM((section_count, width), jnp.int32),
            pltpu.VMEM((1, 2, width), F32),
            pltpu.VMEM((section_count, width), jnp.int32),
            pltpu.VMEM((qubits, micro, batch), jnp.int32),
            pltpu.SemaphoreType.DMA((5,)),
            pltpu.SemaphoreType.DMA((chunks,)),
            pltpu.VMEM((CHUNK * s8, 256), F32),
            pltpu.VMEM((2 * s8, rows * s8), F32),
        ],
        name="stage_a",
    )(*(pltpu.with_memory_space_constraint(x, pltpu.HBM) for x in operands))
    recv = lax.all_to_all(blocks, ("b", "z", "c"), 0, 0, tiled=True)

    pay_rows = z_count * 4 * s8 + 2 * s8 + ROW_TILE
    pay = (section_count, pay_rows, rows)
    keep, send, amps = call(
        functools.partial(second_body, buffers),
        12,
        out_shape=[sds(pay, F32), sds(pay, F32), sds((8, 2 * half), F32)],
        in_specs=[vmem] * (6 + buffers),
        out_specs=[vmem, vmem, vmem],
        scratch_shapes=[
            pltpu.VMEM((2, 4 * half, rows * s8), BF16),
            pltpu.VMEM((4 * half, width), F32),
            pltpu.VMEM((2, 2, 128, width), BF16),
            pltpu.VMEM((4 * s8, rows * s8), F32),
        ],
        name="stage_b",
    )(*held, recv, hot, probe_vectors, own_set, firsts, back_order)
    other = lax.ppermute(send, "c", [(0, 1), (1, 0)])
    packed = call(
        pack_body, 4, out_shape=sds(pay, F32), in_specs=[vmem, vmem], out_specs=vmem, name="pack"
    )(keep, other)
    got = lax.all_to_all(packed, ("a", "b"), 0, 0, tiled=True)
    u_parts = got[1, : z_count * 4 * s8].reshape(z_count, 4 * s8, rows)
    u_recv = lax.all_to_all(u_parts, "z", 0, 0, tiled=True)

    contrib = call(
        functools.partial(final_body, s8),
        8,
        out_shape=sds((section_count * stem_count, 2, count), F32),
        in_specs=[vmem] * 3,
        out_specs=vmem,
        scratch_shapes=[pltpu.VMEM((4 * s8, rows * s8), F32)],
        name="final",
    )(u_recv, got, amps)
    arrived = lax.all_to_all(contrib, ("a", "b", "z", "c"), 0, 0, tiled=True)
    return call(
        total_body,
        4,
        out_shape=sds((1, 2, micro, batch), F32),
        in_specs=[vmem],
        out_specs=vmem,
        name="total",
    )(arrived)


def solution(mesh):
    sections, stems = (mesh.shape[name] for name in ("section", "stem"))
    devices = mesh.devices.reshape(sections // 2, 2, stems // 2, 2)
    fine = Mesh(devices, ("a", "b", "z", "c"))
    return jax.shard_map(
        local,
        mesh=fine,
        in_specs=(
            P(("a", "b")),
            P(),
            P(("a", "b"), None, ("z", "c")),
            P(("a", "b")),
            P(),
        ),
        out_specs=P(("a", "b")),
        check_vma=False,
    )
```

```python
import functools

import jax
import jax.numpy as jnp
from jax import lax
from jax.experimental import pallas as pl
from jax.experimental.pallas import tpu as pltpu
from jax.sharding import Mesh
from jax.sharding import PartitionSpec as P


F32 = jnp.float32
BF16 = jnp.bfloat16
NT = (((1,), (1,)), ((), ()))
CHUNK = 32
TILE = 256
ROW_TILE = 8


def split(x):
    high = x.astype(BF16)
    return high, (x - high.astype(F32)).astype(BF16)


def mm(a, b):
    return jnp.dot(a, b, preferred_element_type=F32)


def mm_nt(a, b):
    return lax.dot_general(a, b, NT, preferred_element_type=F32)


def iota(shape, dim):
    return lax.broadcasted_iota(jnp.int32, shape, dim)


def one_hot(cond):
    return jnp.where(cond, 1.0, 0.0).astype(BF16)


def repeat_matrix(rows, settings):
    shape = (rows, rows * settings)
    return one_hot(iota(shape, 1) // settings == iota(shape, 0))


def position():
    section = lax.axis_index("a") * lax.axis_size("b") + lax.axis_index("b")
    core = lax.axis_index("c")
    rank = lax.axis_index("z") * lax.axis_size("c") + core
    return section, rank, core


def chunk_copy(stem_hbm, bufs, sem, b, i):
    held = bufs[b].shape[1]
    source = stem_hbm.at[0, :, pl.ds(b * held + i * CHUNK, CHUNK)]
    slot = sem.at[b * (held // CHUNK) + i]
    return pltpu.make_async_copy(source, bufs[b].at[:, pl.ds(i * CHUNK, CHUNK)], slot)


def permuted_tiles(parts, hot_ref, store):
    count = parts.shape[0] // 2
    for i in range(0, hot_ref.shape[1], TILE):
        total = mm(parts, hot_ref[:, i : i + TILE])
        store(i, total[:count] + total[count:])


def gathered_tiles(source_ref, order_ref, store):
    count, width = 2 * ROW_TILE, source_ref.shape[1]
    for i in range(0, width, 128):
        index = jnp.broadcast_to(order_ref[0:1, i : i + 128], (ROW_TILE, 128))
        lane, tile = index % 128, index // 128
        pieces = []
        for r in range(0, count, ROW_TILE):
            piece = jnp.zeros((ROW_TILE, 128), F32)
            for t in range(width // 128):
                part = source_ref[r : r + ROW_TILE, 128 * t : 128 * t + 128]
                got = jnp.take_along_axis(part, lane, axis=1, mode="promise_in_bounds")
                piece = jnp.where(tile == t, got, piece)
            pieces.append(piece)
        store(i, jnp.concatenate(pieces, 0))


def probe_amplitudes(probe, vectors):
    ones = jnp.ones((8, 128), BF16)
    sums = [jnp.zeros((vectors.shape[0], 128), F32)] * 2
    for j in range(0, vectors.shape[1], 128):
        part = vectors[:, j : j + 128]
        sums = [s + part * probe[p : p + 1, j : j + 128] for p, s in enumerate(sums)]
    out = []
    for s in sums:
        hi, lo = split(s)
        out.append((mm_nt(ones, hi) + mm_nt(ones, lo))[0:1])
    return jnp.concatenate(out, 0)


def first_body(buffers, boundary_hbm, perm_hbm, stem_hbm, probe_hbm, bits_hbm, block_out, fwd_ref, set_out, back_order_out, hot_out, *rest):
    bufs = rest[:buffers]
    boundary_smem, perm_smem, probe_ref, perm_ref, bits_ref, small, sem, part_ref, back_ref = rest[buffers:]
    section, rank, core = position()
    held, s8, width = bufs[0].shape[1:]
    rows = held * buffers
    per = held // CHUNK
    lanes = CHUNK * s8
    stem_count = block_out.shape[0] // 2
    target = (1 - lax.axis_index("b")) * stem_count
    pairs = [
        (perm_hbm, perm_ref),
        (boundary_hbm, boundary_smem),
        (perm_hbm, perm_smem),
        (probe_hbm, probe_ref),
        (bits_hbm, bits_ref),
    ]
    little = [pltpu.make_async_copy(a, b, small.at[i]) for i, (a, b) in enumerate(pairs)]
    for copy in little:
        copy.start()
    large = [chunk_copy(stem_hbm, bufs, sem, b, i) for b in range(buffers) for i in range(per)]
    large[0].start()
    for copy in little:
        copy.wait()
    for copy in large[1:]:
        copy.start()
    settings = bits_ref[0]
    for q in range(1, bits_ref.shape[0]):
        settings += jnp.left_shift(bits_ref[q], q)
    line = jnp.concatenate([settings[i : i + 1] for i in range(settings.shape[0])], 1)
    set_out[...] = jnp.broadcast_to(line.astype(F32), set_out.shape)

    @pl.when(section == 0)
    def _():
        perm_ref[0:1] = perm_ref[1:2]

    @pl.when(section == 1)
    def _():
        wanted = perm_ref[2:3]
        parts = [wanted[:, d * rows : (d + 1) * rows] for d in range(stem_count)]
        kept_first = [jnp.concatenate(parts[c::2] + parts[1 - c :: 2], 1) for c in (0, 1)]
        row = jnp.where(core == 0, kept_first[0], kept_first[1])
        z, z_count = lax.axis_index("z"), stem_count // 2
        for bit in range((z_count - 1).bit_length()):
            parts = [row[:, d * rows : (d + 1) * rows] for d in range(stem_count)]
            order = [d // z_count * z_count + (d % z_count ^ 1 << bit) for d in range(stem_count)]
            other = jnp.concatenate([parts[d] for d in order], 1)
            row = jnp.where((z >> bit) % 2 == 1, other, row)
        perm_ref[0:1] = row

        def place(i, carry):
            at = pl.ds(pl.multiple_of(i * TILE, TILE), TILE)
            row = perm_ref[0:1, at]
            for j in range(0, width, TILE):
                hot_out[j : j + TILE, at] = one_hot(iota((TILE, TILE), 0) + j == row)
            return carry

        lax.fori_loop(0, width // TILE, place, 0)

    @pl.when(section == 2)
    def _():
        def place(i, carry):
            at = pl.ds(pl.multiple_of(i * 128, 128), 128)
            wanted = jnp.broadcast_to(perm_ref[3:4, at], (128, 128)).astype(F32).T
            for j in range(0, width, 128):
                place_at = (iota((128, 128), 1) + j).astype(F32)
                hot_out[at, j : j + 128] = one_hot(place_at == wanted)
            return carry

        lax.fori_loop(0, width // 128, place, 0)
        number = iota((16, width), 1)
        digits = jnp.where(iota((16, width), 0) == 0, number // 128, number % 128)
        digits = digits.astype(F32).astype(BF16)
        for j in range(0, width, TILE):
            found = mm(digits, hot_out[:, j : j + TILE])
            line = (found[0:1] * 128.0 + found[1:2]).astype(jnp.int32)
            back_order_out[:, j : j + TILE] = jnp.broadcast_to(line, (ROW_TILE, TILE))

    @pl.when((section == 1) | (section == 2))
    def _():
        for b in range(buffers):
            for i in range(per):
                chunk_copy(stem_hbm, bufs, sem, b, i).wait()

    @pl.when(section == 0)
    def _():
        fwd_ref[...] = jnp.zeros(fwd_ref.shape, F32)
        piece = min(width, 1024)

        def chunk(b, c, carry):
            chunk_copy(stem_hbm, bufs, sem, b, c).wait()
            for j in range(0, width, piece):
                at = slice(j, j + piece)

                def one(i, sums):
                    k = c * CHUNK + i
                    source = perm_smem[0, rank * rows + b * held + k]
                    b_re, b_im = boundary_smem[0, source], boundary_smem[1, source]
                    t_re, t_im = bufs[b][0, k, :, at], bufs[b][1, k, :, at]
                    return sums[0] + (b_re * t_re - b_im * t_im), sums[1] + (b_re * t_im + b_im * t_re)

                start = fwd_ref[0:s8, at], fwd_ref[s8:, at]
                done = lax.fori_loop(0, CHUNK, one, start, unroll=4)
                fwd_ref[0:s8, at], fwd_ref[s8:, at] = done
            return carry

        for b in range(buffers):
            lax.fori_loop(0, per, functools.partial(chunk, b), 0)
        def store(i, moved):
            n = min(rows, 128)
            for o in range(0, 128, n):
                dest, lane = divmod(i + o, rows)
                block_out[target + dest, :, lane : lane + n] = moved[:, o : o + n]

        gathered_tiles(fwd_ref, perm_ref, store)

    @pl.when(section == 3)
    def _():
        ones = jnp.ones((s8, 128), BF16)
        quarters = 4
        span = width // 128 // quarters

        def chunk(b, c, carry):
            chunk_copy(stem_hbm, bufs, sem, b, c).wait()
            for q in range(quarters):
                tiles = [slice(128 * t, 128 * t + 128) for t in range(q * span, (q + 1) * span)]
                p_re = [jnp.broadcast_to(probe_ref[0, 0:1, t], (s8, 128)) for t in tiles]
                p_im = [jnp.broadcast_to(probe_ref[0, 1:2, t], (s8, 128)) for t in tiles]

                def one(i, carry):
                    k = c * CHUNK + i
                    re, im = None, None
                    for n, t in enumerate(tiles):
                        t_re, t_im = bufs[b][0, k, :, t], bufs[b][1, k, :, t]
                        r = t_re * p_re[n] - t_im * p_im[n]
                        m = t_re * p_im[n] + t_im * p_re[n]
                        re, im = (r, m) if re is None else (re + r, im + m)
                    at = pl.ds(pl.multiple_of(i * s8, s8), s8)
                    if q == 0:
                        part_ref[at, 0:128], part_ref[at, 128:] = re, im
                    else:
                        part_ref[at, 0:128] += re
                        part_ref[at, 128:] += im
                    return carry

                lax.fori_loop(0, CHUNK, one, 0, unroll=8)
            hi, lo = split(part_ref[...])
            at = pl.ds(pl.multiple_of((b * per + c) * lanes, lanes), lanes)
            for plane in range(2):
                side = slice(128 * plane, 128 * plane + 128)
                back_ref[s8 * plane : s8 * plane + s8, at] = mm_nt(ones, hi[:, side]) + mm_nt(ones, lo[:, side])
            return carry

        for b in range(buffers):
            lax.fori_loop(0, per, functools.partial(chunk, b), 0)
        group = min(rows, 128)
        rep = repeat_matrix(group, s8)
        shape = (2 * s8, group * s8)
        pick = (iota(shape, 1) % s8) == (iota(shape, 0) % s8)
        for start in range(0, rows, group):
            spread = jnp.where(pick, back_ref[:, start * s8 : (start + group) * s8], 0.0)
            hi, lo = split(spread)
            out = mm_nt(hi, rep) + mm_nt(lo, rep)
            for d in range(stem_count):
                block_out[target + d, :, start : start + group] = out


def second_body(buffers, *refs):
    bufs = refs[:buffers]
    recv_ref, hot_ref, probe_ref, set_ref, fwd_ref, order_ref, keep_out, send_out, amp_out = refs[buffers : buffers + 9]
    lhs_ref, acc_ref, back_lhs_ref, back_ref = refs[buffers + 9 :]
    section, _, _ = position()
    held, s8, width = bufs[0].shape[1:]
    rows = held * buffers
    count = rows // CHUNK
    per = held // CHUNK
    lanes = CHUNK * s8
    half = s8 * s8
    stem_count = recv_ref.shape[0] // 2
    body = 4 * s8 * (stem_count // 2)
    source = (1 - lax.axis_index("b")) * stem_count
    group = min(rows, 128)
    batch = set_ref.shape[1]

    for q in range(keep_out.shape[0]):
        for i, at in enumerate(range(0, batch, rows)):
            n = min(rows, batch - at)
            keep_out[q, body + 2 * s8 + i : body + 2 * s8 + i + 1, 0:n] = set_ref[0:1, at : at + n]

    @pl.when(section == 0)
    def _():
        gap = jnp.zeros((s8, width), F32)
        spaced = jnp.concatenate([fwd_ref[:s8], gap, fwd_ref[s8:], gap], 0)
        amp_out[0:2, 0 : 4 * s8] = probe_amplitudes(probe_ref[0], spaced)

    @pl.when(section == 1)
    def _():
        acc_ref[...] = jnp.zeros(acc_ref.shape, F32)
        state = recv_ref[source]
        for d in range(1, stem_count):
            state += recv_ref[source + d]
        rep = repeat_matrix(group, s8)
        mask_shape = (2 * s8, group * s8)
        pick = (iota(mask_shape, 1) % s8) == (iota(mask_shape, 0) % s8)
        upper = iota(mask_shape, 0) < s8
        for start in range(0, rows, group):
            hi, lo = split(state[:, start : start + group])
            wide = mm(jnp.concatenate([hi, lo], 0), rep)
            at = pl.ds(start * s8, group * s8)
            for level in range(2):
                for quarter in range(s8 // 2):
                    base = level * 2 * s8 + 2 * quarter
                    built = []
                    for plane in range(2):
                        r = base + plane * s8
                        value = jnp.where(upper, wide[r : r + 1], wide[r + 1 : r + 2])
                        built.append(jnp.where(pick, value, 0.0))
                    top = level * 2 * half + quarter * 4 * s8
                    lo_rows = pl.ds(top, 2 * s8)
                    hi_rows = pl.ds(top + 2 * s8, 2 * s8)
                    lhs_ref[0, lo_rows, at] = built[0].astype(BF16)
                    lhs_ref[0, hi_rows, at] = built[1].astype(BF16)
                    lhs_ref[1, lo_rows, at] = (-built[1]).astype(BF16)
                    lhs_ref[1, hi_rows, at] = built[0].astype(BF16)

        for c in range(count):
            at = slice(c * lanes, (c + 1) * lanes)
            ks = slice(c % per * CHUNK, (c % per + 1) * CHUNK)
            for j in range(0, width, 2 * TILE):
                cols = slice(j, j + 2 * TILE)
                total = acc_ref[:, cols]
                extra = jnp.zeros((2 * half, 2 * TILE), F32)
                for plane in range(2):
                    hi, lo = split(bufs[c // per][plane, ks, :, cols].reshape(lanes, 2 * TILE))
                    e = lhs_ref[plane, :, at]
                    total += mm(e, hi)
                    extra += mm(e[: 2 * half], lo)
                acc_ref[0 : 2 * half, cols] = total[: 2 * half] + extra
                acc_ref[2 * half :, cols] = total[2 * half :]
        full = acc_ref[0 : 2 * half] + acc_ref[2 * half :]
        amp_out[0:2] = probe_amplitudes(probe_ref[0], full)

        def store(i, moved):
            n = min(rows, TILE)
            for o in range(0, TILE, n):
                slot, lane = divmod(i + o, rows)
                z, ref = slot % (stem_count // 2), (keep_out, send_out)[slot // (stem_count // 2)]
                for q in range(s8 // 2):
                    piece = moved[q * 4 * s8 : (q + 1) * 4 * s8, o : o + n]
                    ref[q, z * 4 * s8 : (z + 1) * 4 * s8, lane : lane + n] = piece

        permuted_tiles(jnp.concatenate(split(full), 0), hot_ref, store)

    @pl.when(section == 2)
    def _():
        zero = jnp.zeros((s8 - 1, width), F32)
        for d in range(stem_count):
            acc_ref[0 : 2 * s8, d * rows : (d + 1) * rows] = recv_ref[source + d]
        moved = []
        gathered_tiles(acc_ref, order_ref, lambda i, x: moved.append(x))
        moved = jnp.concatenate(moved, 1)
        real = jnp.concatenate([moved[:s8], probe_ref[0, 0:1], zero], 0)
        imag = jnp.concatenate([moved[s8:], probe_ref[0, 1:2], zero], 0)
        count = 4 * s8
        blank = jnp.zeros((128 - 2 * count, width), BF16)
        for plane, pair in enumerate([(real, imag), (-imag, real)]):
            hi, lo = split(jnp.concatenate(pair, 0))
            back_lhs_ref[plane, 0] = jnp.concatenate([hi, lo, blank], 0)
            back_lhs_ref[plane, 1] = jnp.concatenate([hi, jnp.zeros(lo.shape, BF16), blank], 0)
        for b in range(buffers):
            total = jnp.zeros((held * s8, 128), F32)
            for plane in range(2):
                for level, part in enumerate(split(bufs[b][plane].reshape(held * s8, width))):
                    total += mm_nt(part, back_lhs_ref[plane, level])
            turned = total.T
            at = slice(b * held * s8, (b + 1) * held * s8)
            back_ref[:, at] = turned[:count] + turned[count : 2 * count]
        for i in range(s8):
            at = slice(i * rows, (i + 1) * rows)
            for q in range(keep_out.shape[0]):
                for plane in range(2):
                    row = 2 * s8 * (i) + plane * s8
                    keep_out[q, row : row + s8, :] = back_ref[2 * s8 * plane : 2 * s8 * plane + s8, at]
                    row = body + 2 * i + plane
                    src = 2 * s8 * plane + s8
                    keep_out[q, row : row + 1, :] = back_ref[src : src + 1, at]


def pack_body(keep_ref, recv_ref, out_ref):
    section, _, _ = position()

    @pl.when(section == 1)
    def _():
        out_ref[...] = keep_ref[...] + recv_ref[...]
        tail = keep_ref.shape[1] - ROW_TILE
        out_ref[:, tail:] = keep_ref[:, tail:]

    @pl.when(section != 1)
    def _():
        out_ref[...] = keep_ref[...]


def final_body(settings, got_ref, amp_ref, *refs):
    s8 = settings
    u_refs, (out_ref, x_ref) = refs[:-2], refs[-2:]
    section, _, _ = position()
    half = s8 * s8
    section_count = got_ref.shape[0]
    rows = got_ref.shape[2]
    count = out_ref.shape[2]
    body = (1 + len(u_refs)) * 4 * s8
    u = got_ref[1, 0 : 4 * s8]
    for u_ref in u_refs:
        u += u_ref[...]
    x_ref[...] = jnp.zeros(x_ref.shape, F32)
    for i in range(s8):
        at = slice(i * rows, (i + 1) * rows)
        for plane in range(2):
            row = 2 * s8 * i + plane * s8
            x_ref[2 * s8 * plane : 2 * s8 * plane + s8, at] = got_ref[2, row : row + s8]
            row = body + 2 * i + plane
            to = 2 * s8 * plane + s8
            x_ref[to : to + 1, at] = got_ref[2, row : row + 1]
    group = min(rows, 128)
    rep = repeat_matrix(group, s8)
    shape = (s8, group * s8)
    pick = (iota(shape, 1) % s8) == iota(shape, 0)
    table = jnp.zeros((4 * s8, 4 * half), F32)
    for start in range(0, rows, group):
        hi, lo = split(u[:, start : start + group])
        wide = mm(jnp.concatenate([hi, lo], 0), rep)
        spread = []
        for level in range(2):
            tiles = [
                jnp.where(pick, wide[r : r + 1], 0.0)
                for r in range(level * 4 * s8, (level + 1) * 4 * s8)
            ]
            spread.append(jnp.concatenate(tiles, 0).astype(BF16))
        x_hi, x_lo = split(x_ref[:, start * s8 : (start + group) * s8])
        both = mm_nt(jnp.concatenate([x_hi, x_lo], 0), spread[0])
        table += both[: 4 * s8] + both[4 * s8 :] + mm_nt(x_hi, spread[1])
    per = 2 * s8 * s8
    re_u, im_u = table[:, :per], table[:, per:]
    c_re = re_u[: 2 * s8] - im_u[2 * s8 :]
    c_im = re_u[2 * s8 :] + im_u[: 2 * s8]
    top = body + 2 * s8
    s = []
    for i in range(section_count):
        pieces = [
            got_ref[i, top + n : top + n + 1, 0 : min(rows, count - at)]
            for n, at in enumerate(range(0, count, rows))
        ]
        s.append(jnp.concatenate(pieces, 1).astype(jnp.int32))
    code = ((s[0] % 2) * s8 + s[1]) * s8 + s[2]
    sel = one_hot((iota((per, count), 0) == code) & (s[0] // 2 == section))
    parts = split(jnp.concatenate([c_re, c_im], 0))
    chosen = mm(parts[0], sel) + mm(parts[1], sel)
    match = iota((s8, count), 0) == s[3]
    result = [[None, None] for _ in range(section_count)]
    for plane in range(2):
        top = plane * 2 * s8
        result[3][plane] = jnp.sum(jnp.where(match, chosen[top : top + s8], 0.0), 0, keepdims=True)
        result[2][plane] = chosen[top + s8 : top + s8 + 1]
    lead = jnp.where(section == 0, 0, s[0])
    ending = jnp.where(section == 0, s[0], s[1])
    place = (lead // 2) * (4 * s8) + (lead % 2) * s8 + ending
    at = iota((2 * half, count), 0)
    valid = iota((8, 2 * half), 1) < jnp.where(section == 0, 4 * s8, 2 * half)
    pair = split(jnp.where(valid & (section < 2), amp_ref[...], 0.0))
    picked = []
    for shift in (0, 2 * s8):
        oh = one_hot(at == place + shift)
        picked.append(mm(pair[0], oh) + mm(pair[1], oh))
    real = picked[0][0:1] - picked[1][1:2]
    imag = picked[0][1:2] + picked[1][0:1]
    for target in (0, 1):
        mine = section == target
        result[target] = [jnp.where(mine, real, 0.0), jnp.where(mine, imag, 0.0)]
    each = out_ref.shape[0] // section_count
    for target in range(section_count):
        pair = jnp.concatenate(result[target], 0)
        for r in range(each):
            out_ref[target * each + r] = pair


def total_body(part_ref, out_ref):
    total = part_ref[0]
    for i in range(1, part_ref.shape[0]):
        total += part_ref[i]
    micro, batch = out_ref.shape[2:]
    for m in range(micro):
        for plane in range(2):
            out_ref[0, plane, m : m + 1] = total[plane : plane + 1, m * batch : (m + 1) * batch]


def local(bitstrings, boundary, stem_tensor, probe_vectors, inbound_permutations):
    rows, s8, width = stem_tensor.shape[2:]
    micro, batch, qubits = bitstrings.shape[1:]
    count = micro * batch
    section_count = lax.axis_size("a") * lax.axis_size("b")
    z_count = lax.axis_size("z")
    stem_count = z_count * lax.axis_size("c")
    assert section_count == 4 and s8 == 2 * section_count
    half = s8 * s8
    sds = jax.ShapeDtypeStruct
    vmem = pl.BlockSpec(memory_space=pltpu.VMEM)
    smem = pl.BlockSpec(memory_space=pltpu.SMEM)
    hbm = pl.BlockSpec(memory_space=pltpu.HBM)
    operands = boundary, inbound_permutations, stem_tensor, probe_vectors, bitstrings[0].transpose(2, 0, 1)
    chunks = rows // CHUNK
    buffers = min(4, chunks)

    def call(body, limit, **kwargs):
        params = pltpu.CompilerParams(vmem_limit_bytes=limit * 2**20)
        return pl.pallas_call(body, compiler_params=params, **kwargs)

    blocks, firsts, own_set, back_order, hot, *held = call(
        functools.partial(first_body, buffers),
        8,
        out_shape=[
            sds((2 * stem_count, 2 * s8, rows), F32),
            pltpu.VMEM((2 * s8, width), F32),
            sds((8, count), F32),
            sds((ROW_TILE, width), jnp.int32),
            pltpu.VMEM((width, width), BF16),
        ]
        + [pltpu.VMEM((2, rows // buffers, s8, width), F32)] * buffers,
        in_specs=[hbm] * 5,
        out_specs=[vmem] * (5 + buffers),
        scratch_shapes=[
            pltpu.SMEM((2, width), F32),
            pltpu.SMEM((section_count, width), jnp.int32),
            pltpu.VMEM((1, 2, width), F32),
            pltpu.VMEM((section_count, width), jnp.int32),
            pltpu.VMEM((qubits, micro, batch), jnp.int32),
            pltpu.SemaphoreType.DMA((5,)),
            pltpu.SemaphoreType.DMA((chunks,)),
            pltpu.VMEM((CHUNK * s8, 256), F32),
            pltpu.VMEM((2 * s8, rows * s8), F32),
        ],
        name="stage_a",
    )(*(pltpu.with_memory_space_constraint(x, pltpu.HBM) for x in operands))
    recv = lax.all_to_all(blocks, ("b", "z", "c"), 0, 0, tiled=True)

    pay_rows = z_count * 4 * s8 + 2 * s8 + ROW_TILE
    pay = (section_count, pay_rows, rows)
    keep, send, amps = call(
        functools.partial(second_body, buffers),
        12,
        out_shape=[sds(pay, F32), sds(pay, F32), sds((8, 2 * half), F32)],
        in_specs=[vmem] * (6 + buffers),
        out_specs=[vmem, vmem, vmem],
        scratch_shapes=[
            pltpu.VMEM((2, 4 * half, rows * s8), BF16),
            pltpu.VMEM((4 * half, width), F32),
            pltpu.VMEM((2, 2, 128, width), BF16),
            pltpu.VMEM((4 * s8, rows * s8), F32),
        ],
        name="stage_b",
    )(*held, recv, hot, probe_vectors, own_set, firsts, back_order)
    other = lax.ppermute(send, "c", [(0, 1), (1, 0)])
    packed = call(
        pack_body, 4, out_shape=sds(pay, F32), in_specs=[vmem, vmem], out_specs=vmem, name="pack"
    )(keep, other)
    got = lax.all_to_all(packed, ("a", "b"), 0, 0, tiled=True)
    u_recv = []
    for i in range(1, z_count):
        route = [(j, j ^ i) for j in range(z_count)]
        u_recv.append(lax.ppermute(got[1, i * 4 * s8 : (i + 1) * 4 * s8], "z", route))

    contrib = call(
        functools.partial(final_body, s8),
        8,
        out_shape=sds((section_count * stem_count, 2, count), F32),
        in_specs=[vmem] * (1 + z_count),
        out_specs=vmem,
        scratch_shapes=[pltpu.VMEM((4 * s8, rows * s8), F32)],
        name="final",
    )(got, amps, *u_recv)
    arrived = lax.all_to_all(contrib, ("a", "b", "z", "c"), 0, 0, tiled=True)
    return call(
        total_body,
        4,
        out_shape=sds((1, 2, micro, batch), F32),
        in_specs=[vmem],
        out_specs=vmem,
        name="total",
    )(arrived)


def solution(mesh):
    sections, stems = (mesh.shape[name] for name in ("section", "stem"))
    devices = mesh.devices.reshape(sections // 2, 2, stems // 2, 2)
    fine = Mesh(devices, ("a", "b", "z", "c"))
    return jax.shard_map(
        local,
        mesh=fine,
        in_specs=(
            P(("a", "b")),
            P(),
            P(("a", "b"), None, ("z", "c")),
            P(("a", "b")),
            P(),
        ),
        out_specs=P(("a", "b")),
        check_vma=False,
    )
```
